32 devices in a mesh: lat: 8 (over z, y), lon: 4 (over x, core).
Axes of the slice: x: 2, y: 2, z: 4, core: 2. Of those that a mesh axis runs over, the one named last changes fastest.
Arguments:
- field: bfloat16 [150, 128, 1024], P(None, 'lat', 'lon'), may hold values from -6 to 6
- land_mask: int32 [128, 1024], P('lat', 'lon'), may hold values 0 or 1
- fold_partner: int32 [1024], replicated, may hold values from 0 to 1023, as said below
- dw_kernel: float32 [150, 7, 7], replicated, may hold values from -0.875 to 0.875
- norm_gain: float32 [150], replicated, may hold values from 0.1 to 1.9
- w_in: bfloat16 [150, 600], replicated, may hold values from -0.5 to 0.5
- w_out: bfloat16 [600, 150], replicated, may hold values from -0.25 to 0.25
- spec_gain: float32 [2, 150, 512], replicated, may hold values from -12 to 12
- mix_weight: bfloat16 [150, 150], replicated, may hold values from -0.5 to 0.5
Outputs:
- block_out: bfloat16 [150, 128, 1024], P(None, 'lat', 'lon')
The draws below stay inside these ranges and needn't reach their ends.
Inputs may be any that keep to these rules, and one draw needn't show every extreme that they name: There is one s such that fold_partner[j] = (s - j) mod 1024 for every j.
All inputs are finite; a program needn't handle non-finite values. No bound on the sum of `land_mask` on one device may be relied on, other than what follows from the above.
Results may differ from the reference program's by a relative error of at most 0.0065.
Values may be sent and summed in bfloat16 or wider, within the bound.
A program may use at most 128 MiB of HBM per device.

```python
import math
import jax
import jax.numpy as jnp
from jax import lax

C = 150
HID = 600
M = 512
RL = 16
NLAT = 128
LON = 1024


def draw_fold_partner(key, part):
    pivot_at = jax.random.randint(jax.random.fold_in(key, 11), (), 0, LON, dtype=jnp.int32)
    return ((pivot_at - jnp.arange(LON, dtype=jnp.int32)) % LON).astype(jnp.int32)


def plant(drawn, stream_key, low, largest):
    spot = [jax.random.randint(jax.random.fold_in(stream_key, axis), (), 0, length) for axis, length in enumerate(drawn.shape)]
    widest = drawn.shape.index(max(drawn.shape))
    neighbour = spot[:widest] + [(spot[widest] + 1) % drawn.shape[widest]] + spot[widest + 1:]
    return drawn.at[tuple(spot)].set(low).at[tuple(neighbour)].set(largest)


def levels(own_key, dims, split, low, top_value):
    gain = 1.0
    for axis_at, blocks in split:
        draws = jax.random.uniform(jax.random.fold_in(jax.random.fold_in(own_key, 6), axis_at), (blocks,), jnp.float32, low / len(split), top_value / len(split))
        gain = gain * jnp.repeat(jnp.exp(draws), dims[axis_at] // blocks).reshape((-1,) + (1,) * (len(dims) - 1 - axis_at))
    return gain


def bell_draw(key, dims, width, bound, shards=(), kind=jnp.bfloat16):
    drawn = width * jax.random.normal(key, dims, jnp.float32)
    if shards:
        drawn = drawn * levels(key, dims, shards, -0.22, 0.18)
    return jnp.clip(drawn, -bound, bound).astype(kind)


def setup_inputs(seed: int = 0) -> dict:
    keys = jax.random.split(jax.random.key(seed), 10)
    field = bell_draw(keys[0], (C, NLAT, LON), 1.0, 6.0, ((1, 8), (2, 4)))
    land_mask = plant((jax.random.randint(keys[1], (NLAT, LON), 0, 4) < 3).astype(jnp.int32), jax.random.fold_in(keys[1], 1), 0, 1)
    fold_partner = draw_fold_partner(jax.random.fold_in(keys[9], 71), 0)
    dw_kernel = bell_draw(keys[3], (C, 7, 7), 49 ** -0.5, 0.875, (), jnp.float32)
    norm_gain = jnp.clip(1.0 + 0.18 * jax.random.normal(keys[4], (C,), jnp.float32), 0.1, 1.9)
    w_in = bell_draw(keys[5], (C, HID), C ** -0.5, 0.5)
    w_out = bell_draw(keys[6], (HID, C), HID ** -0.5, 0.25)
    spec_gain = bell_draw(keys[7], (2, C, M), 2.0, 12.0, (), jnp.float32)
    mix_weight = bell_draw(keys[8], (C, C), C ** -0.5, 0.5)
    return {"field": field, "land_mask": land_mask, "fold_partner": fold_partner, "dw_kernel": dw_kernel, "norm_gain": norm_gain, "w_in": w_in, "w_out": w_out, "spec_gain": spec_gain, "mix_weight": mix_weight}


def dft_table(lon_points, mode_count, first_col, col_count):
    points = first_col + jnp.arange(col_count, dtype=jnp.int32)
    freqs = jnp.arange(mode_count, dtype=jnp.int32)
    phase_index = points[:, None] * freqs[None, :] % lon_points
    angles = phase_index.astype(jnp.float32) * (2.0 * math.pi / lon_points)
    factor = 1.0 / math.sqrt(lon_points)
    return jnp.concatenate([jnp.cos(angles) * factor, -jnp.sin(angles) * factor], axis=1).astype(jnp.bfloat16)

def apply_gain(spectrum, spec_gain, mode_count):
    spec_re = spectrum[..., :mode_count]
    spec_im = spectrum[..., mode_count:]
    gain_re = spec_gain[0][:, None, :]
    gain_im = spec_gain[1][:, None, :]
    return jnp.concatenate([gain_re * spec_re - gain_im * spec_im, gain_re * spec_im + gain_im * spec_re], axis=-1).astype(jnp.bfloat16)

def reference(field, land_mask, fold_partner, dw_kernel, norm_gain, w_in, w_out, spec_gain, mix_weight):
    wet_grid = land_mask.astype(field.dtype)
    masked = field * wet_grid[None]
    columns = (jnp.arange(LON + 6, dtype=jnp.int32) - 3) % LON
    lon_padded = jnp.take(masked, columns, axis=2)
    ghost_rows = jnp.take(masked[:, NLAT - 3:, :][:, ::-1, :], jnp.take(fold_partner, columns), axis=1 + 1)
    south_rows = jnp.zeros((C, 3, LON + 6), field.dtype)
    extended = jnp.concatenate([south_rows, lon_padded, ghost_rows], axis=1)
    fourier = dft_table(LON, M, 0, LON).astype(jnp.float32)
    w_in32 = w_in.astype(jnp.float32)
    w_out32 = w_out.astype(jnp.float32)
    mix32 = mix_weight.astype(jnp.float32)

    def row_block(block_index, result):
        offset = (block_index * RL).astype(jnp.int32)
        tile_rows = lax.dynamic_slice_in_dim(extended, offset, RL + 6, 1)
        depth = jnp.zeros((C, RL, LON), jnp.float32)
        for tap_row in range(7):
            for tap_col in range(7):
                weight_col = dw_kernel[:, tap_row, tap_col][:, None, None]
                depth = depth + weight_col * tile_rows[:, tap_row:tap_row + RL, tap_col:tap_col + LON].astype(jnp.float32)
        masked_rows = lax.dynamic_slice_in_dim(masked, offset, RL, 1).reshape(C, -1).astype(jnp.float32)
        wet_rows = lax.dynamic_slice_in_dim(wet_grid, offset, RL, 0).reshape(1, -1).astype(jnp.float32)
        flat = depth.reshape(C, -1)
        average = lax.optimization_barrier(jnp.mean(flat, axis=0, keepdims=True))
        centred = flat - average
        variance = lax.optimization_barrier(jnp.mean(centred * centred, axis=0, keepdims=True))
        normed = (centred * lax.rsqrt(variance + 1e-06) * norm_gain[:, None]).astype(jnp.bfloat16)
        pre_act = jnp.einsum('ch,cp->hp', w_in32, normed.astype(jnp.float32))
        hidden = jax.nn.gelu(pre_act, approximate=True).astype(jnp.bfloat16)
        branch = jnp.einsum('hc,hp->cp', w_out32, hidden.astype(jnp.float32))
        residual = (wet_rows * (masked_rows + branch)).astype(jnp.bfloat16)
        spectrum = jnp.dot(residual.reshape(C * RL, LON).astype(jnp.float32), fourier, preferred_element_type=jnp.float32)
        scaled = apply_gain(spectrum.reshape(C, RL, 2 * M), spec_gain, M)
        spatial = jnp.dot(scaled.reshape(C * RL, 2 * M).astype(jnp.float32), fourier.T, preferred_element_type=jnp.float32)
        spatial = spatial.astype(jnp.bfloat16).reshape(C, RL * LON)
        mixed = jnp.einsum('cd,cp->dp', mix32, spatial.astype(jnp.float32))
        output = (wet_rows * (residual.astype(jnp.float32) + mixed)).astype(jnp.bfloat16).reshape(C, RL, LON)
        return lax.dynamic_update_slice_in_dim(result, output, offset, 1)
    return lax.fori_loop(0, NLAT // RL, row_block, jnp.zeros(field.shape, jnp.bfloat16))
```

```python
import functools
import math

import jax
import jax.numpy as jnp
import numpy as np
from jax import lax
from jax.experimental import pallas as pl
from jax.experimental.pallas import tpu as pltpu
from jax.sharding import PartitionSpec as P

F32 = jnp.float32
BF16 = jnp.bfloat16
TAPS = 7
HALO = 3
LANES = 128
WORK = BF16
VMEM_LIMIT = 58 * 1024 * 1024


def dft_table(lon_points, mode_count):
    phase = np.arange(lon_points)[:, None] * np.arange(mode_count)[None, :] % lon_points
    angles = phase.astype(np.float32) * np.float32(2.0 * math.pi / lon_points)
    factor = np.float32(1.0 / math.sqrt(lon_points))
    angles = angles.astype(np.float64)
    table = np.concatenate([np.cos(angles), -np.sin(angles)], axis=1).astype(np.float32)
    return (table * factor).astype(BF16)


def kernel(
    sizes,
    field_hbm, mask_hbm, fold_hbm, taps_hbm, gain_hbm, w_in_hbm, w_out_hbm, mix_hbm, spec_hbm, table_hbm,
    out_ref,
    field_ref, mask_ref, fold_ref, taps_ref, gain_ref, w_in_ref, w_out_ref, mix_ref, spec_raw, table_ref,
    flat, own, depth, flat_out, halo, toep, pattern_t, pattern, pattern_back, edge32, comb32,
    res, by_rows, back, spatial,
    edge_mine, edge_left, edge_right, comb, comb_n, comb_s, rows_n, rows_s, top_all,
    spec_ref, w_in_t, w_out_t, mix_t, gain_col,
    local_sem, edge_send, edge_recv, comb_send, comb_recv, rows_send, rows_recv,
    fold_send, fold_recv, out_send, out_recv, in_send, in_recv,
):
    channels, rows, cols, lat_n, lon_n, modes = sizes
    lon_points = cols * lon_n
    tiles = cols // LANES
    per = rows // lon_n
    step = max(u for u in range(1, 11) if channels % u == 0)
    lat = lax.axis_index("lat")
    lon = lax.axis_index("lon")
    left = lax.rem(lon + lon_n - 1, lon_n)
    right = lax.rem(lon + 1, lon_n)
    chip = lon // 2
    core = lax.rem(lon, 2)
    chips = lon_n // 2
    mate_core = chip * 2 + 1 - core

    def target(k):
        return lax.rem(chip + k // 2, chips) * 2 + lax.rem(core + lax.rem(k, 2), 2)

    def source(k):
        return lax.rem(chip + chips - k // 2, chips) * 2 + lax.rem(core + lax.rem(k, 2), 2)

    pairs = (
        (mask_hbm, mask_ref), (field_hbm, field_ref), (taps_hbm, taps_ref), (fold_hbm, fold_ref), (gain_hbm, gain_ref),
        (w_in_hbm, w_in_ref), (w_out_hbm, w_out_ref), (mix_hbm, mix_ref), (spec_hbm, spec_raw), (table_hbm, table_ref))
    loads = [pltpu.make_async_copy(a, b, local_sem.at[n]) for n, (a, b) in enumerate(pairs)]
    loads[0].start()
    loads[1].start()

    barrier = pltpu.get_barrier_semaphore()
    for k in range(1, lon_n):
        pl.semaphore_signal(barrier, inc=1, device_id={"lon": target(k)})

    @pl.when(lat > 0)
    def _():
        pl.semaphore_signal(barrier, inc=1, device_id={"lat": lat - 1})

    @pl.when(lat < lat_n - 1)
    def _():
        pl.semaphore_signal(barrier, inc=1, device_id={"lat": lat + 1})

    for load in loads[2:]:
        load.start()

    lane = lax.broadcasted_iota(jnp.int32, (rows, LANES), 1)
    loads[0].wait()
    loads[1].wait()
    wet = mask_ref[...].astype(F32)

    @pl.loop(0, channels // step)
    def _(group):
        for u in range(step):
            c = group * step + u
            val = field_ref[c].astype(F32) * wet
            at = pl.multiple_of(c * rows, rows)
            parts = [val[:, h * LANES : (h + 1) * LANES] for h in range(tiles)]
            for h in range(tiles):
                flat[h, pl.ds(at, rows), :] = parts[h]
            edge = jnp.where(lane < HALO, parts[0], jnp.where(lane >= LANES - HALO, parts[-1], 0.0))
            edge = pltpu.roll(edge, 0, 1, stride=8, stride_axis=0)
            edge32[pl.ds(c, 1), :] = jnp.sum(edge, axis=0, keepdims=True)

    edge_mine[...] = edge32[...].astype(BF16)

    count = lon_n - 1 + jnp.where(lat > 0, 1, 0) + jnp.where(lat < lat_n - 1, 1, 0)
    pl.semaphore_wait(barrier, count)

    to_left = pltpu.make_async_remote_copy(
        edge_mine, edge_right, edge_send.at[0], edge_recv.at[0], device_id={"lon": left})
    to_right = pltpu.make_async_remote_copy(
        edge_mine, edge_left, edge_send.at[1], edge_recv.at[1], device_id={"lon": right})
    to_left.start()
    to_right.start()

    def own_row(i):
        for h in range(tiles):
            own[i, :, h * LANES : (h + 1) * LANES] = flat[h, pl.ds(i, channels, stride=rows), :].astype(BF16)

    rows_down = pltpu.make_async_remote_copy(
        own.at[pl.ds(0, HALO)], rows_n, rows_send.at[0], rows_recv.at[0], device_id={"lat": lat - 1})
    rows_up = pltpu.make_async_remote_copy(
        own.at[pl.ds(rows - HALO, HALO)], rows_s, rows_send.at[1], rows_recv.at[1], device_id={"lat": lat + 1})
    comb_down = pltpu.make_async_remote_copy(
        comb, comb_n, comb_send.at[0], comb_recv.at[0], device_id={"lat": lat - 1})
    comb_up = pltpu.make_async_remote_copy(
        comb, comb_s, comb_send.at[1], comb_recv.at[1], device_id={"lat": lat + 1})

    def piece(pos):
        return top_all.at[:, :, pl.ds(pl.multiple_of(pos * cols, LANES), cols)]

    def fold_out(j):
        whom = mate_core if j == 0 else lax.rem(chip + j, chips) * 2 + core
        return pltpu.make_async_remote_copy(
            own.at[pl.ds(rows - HALO, HALO)], piece(lon), fold_send.at[j], fold_recv.at[j], device_id={"lon": whom})

    def fold_pass(j):
        pos = lax.rem(chip + chips - j, chips) * 2 + core
        return pltpu.make_async_remote_copy(
            piece(pos), piece(pos), fold_send.at[chips + j - 1], fold_recv.at[chips + j - 1], device_id={"lon": mate_core})

    for i in range(rows - HALO, rows):
        own_row(i)

    @pl.when(lat < lat_n - 1)
    def _():
        rows_up.start()

    @pl.when(lat == lat_n - 1)
    def _():
        for j in range(chips - 1, -1, -1):
            fold_out(j).start()
        top_all[:, :, pl.ds(pl.multiple_of(lon * cols, LANES), cols)] = own[rows - HALO :]

    for i in range(HALO):
        own_row(i)

    @pl.when(lat > 0)
    def _():
        rows_down.start()

    loads[2].wait()
    pattern_t[...] = jnp.zeros(pattern_t.shape, F32)
    for a in range(TAPS):
        for b in range(TAPS):
            pattern_t[b * rows + a : b * rows + a + 1, :channels] = taps_ref[a, b : b + 1, :]
    pattern[...] = pattern_t[...].T[:channels]
    pattern_back[...] = pltpu.roll(pattern[...], LANES - HALO, 1)

    slot = lax.rem(lane, rows)
    index = lax.broadcasted_iota(jnp.int32, (rows, LANES), 0)
    band = jnp.abs(slot - index) <= HALO
    half = rows // 2
    low_slot = slot[:half] < HALO
    high_slot = (slot[:half] >= half + HALO) & (slot[:half] < half + 2 * HALO)

    @pl.loop(0, channels // step)
    def _(group):
        for u in range(step):
            c = group * step + u
            row = jnp.broadcast_to(pattern_back[pl.ds(c, 1), :], (rows, LANES))
            mid = jnp.where(band, pltpu.roll(row, 0, 1, stride=1, stride_axis=0), 0.0)
            row = jnp.broadcast_to(pattern[pl.ds(c, 1), :], (half, LANES))
            far = pltpu.roll(row, 0, 1, stride=1, stride_axis=0)
            far = jnp.concatenate([jnp.where(low_slot, far, 0.0), jnp.where(high_slot, far, 0.0)], axis=0)
            for n, part in enumerate((mid, far)):
                coarse = part.astype(BF16)
                toep[c, 2 * n * rows : (2 * n + 1) * rows, :] = coarse
                toep[c, (2 * n + 1) * rows : (2 * n + 2) * rows, :] = (part - coarse.astype(F32)).astype(BF16)

    halo[...] = jnp.zeros(halo.shape, F32)

    for i in range(HALO, rows - HALO):
        own_row(i)

    def turned(ref, target_ref):
        n, m = ref.shape
        up = [-(-d // LANES) * LANES for d in (n, m)]
        full = jnp.concatenate([ref[...].astype(F32), jnp.zeros((n, up[1] - m), F32)], axis=1)
        full = jnp.concatenate([full, jnp.zeros((up[0] - n, up[1]), F32)], axis=0)
        target_ref[...] = full.T[: target_ref.shape[0], : target_ref.shape[1]].astype(BF16)

    to_left.wait()
    to_right.wait()
    near = lax.rem(lax.broadcasted_iota(jnp.int32, (channels, LANES), 1), 8) < 4
    both = jnp.where(near, edge_right[...].astype(F32), edge_left[...].astype(F32))
    comb[...] = both.astype(BF16)
    comb32[...] = both

    @pl.when(lat > 0)
    def _():
        comb_down.start()

    @pl.when(lat < lat_n - 1)
    def _():
        comb_up.start()

    def shifted(ring):
        blocks = []
        for b in range(TAPS):
            d = b - HALO
            line = []
            for h in range(tiles):
                if d == 0:
                    line.append(ring[h])
                elif d > 0:
                    line.append(pltpu.roll(jnp.where(lane < d, ring[h + 1], ring[h]), LANES - d, 1))
                else:
                    line.append(pltpu.roll(jnp.where(lane >= LANES + d, ring[h - 1], ring[h]), -d, 1))
            blocks.append(jnp.concatenate(line, axis=1).astype(BF16))
        return jnp.concatenate(blocks, axis=0)

    def product(c, which, ring):
        weights = toep[c, 2 * which * rows : 2 * (which + 1) * rows, : TAPS * rows]
        total = jnp.dot(weights, shifted(ring), preferred_element_type=F32)
        return total[:rows] + total[rows:]

    @pl.loop(0, channels // step)
    def _(group):
        for u in range(step):
            c = group * step + u
            rim = jnp.broadcast_to(comb32[pl.ds(c, 1), :], (half, LANES))
            for bit in (1, 2, 4):
                rim = jnp.where(lax.rem(index[:half] // bit, 2) == 1, pltpu.roll(rim, LANES - 8 * bit, 1), rim)
            rim = jnp.concatenate([rim, pltpu.roll(rim, LANES - 8 * half, 1)], axis=0)
            at = pl.multiple_of(c * rows, rows)
            ring = [flat[h, pl.ds(at, rows), :].astype(WORK) for h in range(tiles)] + [rim.astype(WORK)]
            total = product(c, 0, ring)
            for h in range(tiles):
                depth[h, pl.ds(at, rows), :] = total[:, h * LANES : (h + 1) * LANES]

    for n in range(5, 8):
        loads[n].wait()
    loads[4].wait()
    turned(w_in_ref, w_in_t)
    w_out_t[...] = jnp.zeros(w_out_t.shape, BF16)
    w_out_t[:, : w_out_ref.shape[1]] = w_out_ref[...]
    turned(mix_ref, mix_t)
    diagonal = lax.broadcasted_iota(jnp.int32, (channels, channels), 0) == lax.broadcasted_iota(
        jnp.int32, (channels, channels), 1)
    gain_col[...] = jnp.broadcast_to(
        jnp.sum(jnp.where(diagonal, gain_ref[...], 0.0), axis=1, keepdims=True), (channels, LANES))

    def edges_of(packed, i):
        return pltpu.roll(packed, LANES - 8 * i, 1) if i else packed

    def put_halo(at, value, rim):
        for h in range(tiles):
            halo[h, pl.ds(at, channels, stride=half), :] = value[:, h * LANES : (h + 1) * LANES]
        halo[tiles, pl.ds(at, channels, stride=half), :] = rim

    def await_halo():
        loads[3].wait()

        @pl.when(lat > 0)
        def _():
            rows_down.wait_send()
            comb_down.wait_send()
            rows_up.wait_recv()
            comb_up.wait_recv()
            for r in range(HALO):
                put_halo(r, rows_s[r].astype(F32), edges_of(comb_s[...].astype(F32), rows - HALO + r))

        @pl.when(lat < lat_n - 1)
        def _():
            rows_up.wait_send()
            comb_up.wait_send()
            rows_down.wait_recv()
            comb_down.wait_recv()
            for r in range(HALO):
                put_halo(HALO + r, rows_n[r].astype(F32), edges_of(comb_n[...].astype(F32), r))

        @pl.when(lat == lat_n - 1)
        def _():
            for j in range(1, chips):
                fold_out(j).wait_recv()
                fold_pass(j).start()
            for j in range(chips):
                fold_out(j).wait_send()
            fold_out(0).wait_recv()
            for j in range(1, chips):
                fold_pass(j).wait()
            point = lax.broadcasted_iota(jnp.int32, (lon_points, cols + LANES), 0)
            at = lax.broadcasted_iota(jnp.int32, (1, cols + LANES), 1)
            at = jnp.where(at < cols + HALO, at, at - (cols + LANES)) + lon * cols
            mate = fold_ref[:, :1] - at
            mate = jnp.where(mate < 0, mate + lon_points, mate)
            mate = jnp.where(mate < 0, mate + lon_points, mate)
            mate = jnp.where(mate >= lon_points, mate - lon_points, mate)
            pick = jnp.where(point == mate, 1.0, 0.0).astype(BF16)
            for r in range(HALO):
                row = jnp.dot(top_all[HALO - 1 - r], pick, preferred_element_type=F32)
                put_halo(HALO + r, row[:, :cols], row[:, cols:])

        @pl.loop(0, channels // step)
        def _(group):
            for u in range(step):
                c = group * step + u
                spot = pl.ds(pl.multiple_of(c * half, half), half)
                ring = [jnp.concatenate([halo[h, spot, :]] * 2, axis=0).astype(WORK) for h in range(tiles + 1)]
                total = product(c, 1, ring)
                at = pl.multiple_of(c * rows, rows)
                for h in range(tiles):
                    depth[h, pl.ds(at, rows), :] += total[:, h * LANES : (h + 1) * LANES]

    here = pl.ds(pl.multiple_of(lon * cols, LANES), cols)

    def row_at(chunk, q):
        return lax.rem(chunk * lon_n + q + HALO, rows)

    def send_row(chunk, k):
        s = chunk * (lon_n - 1) + lon_n - 1 - k
        return pltpu.make_async_remote_copy(
            res.at[row_at(chunk, target(k))], by_rows.at[chunk, :, here],
            out_send.at[s], out_recv.at[s], device_id={"lon": target(k)})

    def send_back(chunk, k):
        q = target(k)
        s = chunk * (lon_n - 1) + lon_n - 1 - k
        return pltpu.make_async_remote_copy(
            back.at[chunk, :, pl.ds(pl.multiple_of(q * cols, LANES), cols)], spatial.at[chunk * lon_n + lon],
            in_send.at[s], in_recv.at[s], device_id={"lon": q})

    def mix_rows(chunk):
        @pl.loop(0, lon_n // 2)
        def _(pair):
            k = lon_n - 1 - 2 * pair
            one, two = row_at(chunk, target(k)), row_at(chunk, target(k - 1))
            x = jnp.concatenate(
                [depth[h, pl.ds(row, channels, stride=rows), :] for row in (one, two) for h in range(tiles)], axis=1)
            mean = jnp.sum(x, axis=0, keepdims=True) * (1.0 / channels)
            centred = x - mean
            var = jnp.sum(centred * centred, axis=0, keepdims=True) * (1.0 / channels)
            gain = jnp.concatenate([gain_col[...]] * (2 * tiles), axis=1)
            normed = (centred * lax.rsqrt(var + 1e-06) * gain).astype(BF16)
            pre = jnp.dot(w_in_t[...], normed, preferred_element_type=F32)
            hidden = jax.nn.gelu(pre, approximate=True).astype(BF16)
            branch = jnp.dot(w_out_t[...], hidden, preferred_element_type=F32)
            for n, row in enumerate((one, two)):
                wet_row = mask_ref[pl.ds(row, 1), :].astype(F32)
                part = branch[:, n * cols : (n + 1) * cols]
                res[row] = (wet_row * (own[row].astype(F32) + part)).astype(BF16)
            send_row(chunk, k).start()

            @pl.when(pair < lon_n // 2 - 1)
            def _():
                send_row(chunk, k - 1).start()

            @pl.when(pair == lon_n // 2 - 1)
            def _():
                by_rows[chunk, :, here] = res[two]

    def spectral(chunk):
        for k in range(lon_n - 1, 0, -1):
            send_row(chunk, k).wait_recv()
        spectrum = jnp.dot(by_rows[chunk], table_ref[...], preferred_element_type=F32)
        s_re = spectrum[:, :modes]
        s_im = spectrum[:, modes:]
        g_re = spec_ref[0]
        g_im = spec_ref[1]
        scaled = jnp.concatenate(
            [(g_re * s_re - g_im * s_im).astype(BF16), (g_re * s_im + g_im * s_re).astype(BF16)], axis=1)
        back[chunk] = lax.dot_general(
            scaled, table_ref[...], (((1,), (1,)), ((), ())), preferred_element_type=F32).astype(BF16)
        for k in range(lon_n - 1, 0, -1):
            send_back(chunk, k).start()
        spatial[chunk * lon_n + lon] = back[chunk, :, here]

    def finish(chunk):
        @pl.loop(0, lon_n)
        def _(k):
            @pl.when(k > 0)
            def _():
                send_back(chunk, k).wait_recv()

            pos = source(k)
            row = row_at(chunk, pos)
            mixed = jnp.dot(mix_t[...], spatial[chunk * lon_n + pos], preferred_element_type=F32)
            wet_row = mask_ref[pl.ds(row, 1), :].astype(F32)
            val = wet_row * (res[row].astype(F32) + mixed)
            for h in range(tiles):
                flat_out[h, pl.ds(row, channels, stride=rows), :] = val[:, h * LANES : (h + 1) * LANES]

    halo_done = False
    for chunk in range(per):
        out_rows = [(chunk * lon_n + q + HALO) % rows for q in range(lon_n)]
        if not halo_done and (min(out_rows) < HALO or max(out_rows) >= rows - HALO):
            await_halo()
            halo_done = True
        mix_rows(chunk)

    loads[8].wait()
    wide = modes // LANES
    for p in range(2):
        for t in range(wide):
            spec_ref[p, :, t * LANES : (t + 1) * LANES] = spec_raw[pl.ds(2 * t + p, channels, stride=2 * wide), :]
    loads[9].wait()

    for chunk in range(per):
        spectral(chunk)
    for chunk in range(per):
        finish(chunk)

    @pl.loop(0, channels // step)
    def _(group):
        for u in range(step):
            c = group * step + u
            at = pl.multiple_of(c * rows, rows)
            for h in range(tiles):
                out_ref[c, :, h * LANES : (h + 1) * LANES] = flat_out[h, pl.ds(at, rows), :].astype(BF16)

    for chunk in range(per):
        for k in range(lon_n - 1, 0, -1):
            send_row(chunk, k).wait_send()
            send_back(chunk, k).wait_send()


def local(lat_n, lon_n, field, land_mask, fold_partner, dw_kernel, norm_gain, w_in, w_out, spec_gain, mix_weight):
    channels, rows, cols = field.shape
    modes = spec_gain.shape[2]
    hid = w_in.shape[1]
    lon_points = cols * lon_n
    hid_up = -(-hid // 16) * 16
    chan_up = -(-channels // LANES) * LANES
    tiles = cols // LANES
    table = jnp.asarray(dft_table(lon_points, modes))
    taps = dw_kernel.transpose(1, 2, 0)
    wide = modes // LANES
    spec = spec_gain.transpose(1, 0, 2).reshape(channels, 2, wide, LANES).transpose(0, 2, 1, 3).reshape(-1, LANES)
    per = rows // lon_n
    sizes = (channels, rows, cols, lat_n, lon_n, modes)
    operands = (field, land_mask, fold_partner[None, :], taps, norm_gain[None, :], w_in, w_out.T, mix_weight, spec, table)
    dma = pltpu.SemaphoreType.DMA
    peers = lon_n - 1
    return pl.pallas_call(
        functools.partial(kernel, sizes),
        out_shape=jax.ShapeDtypeStruct(field.shape, BF16),
        in_specs=[pl.BlockSpec(memory_space=pltpu.HBM)] * len(operands),
        out_specs=pl.BlockSpec(memory_space=pltpu.VMEM),
        scratch_shapes=[
            *[pltpu.VMEM(x.shape, x.dtype) for x in operands],
            pltpu.VMEM((tiles, channels * rows, LANES), F32),
            pltpu.VMEM((rows, channels, cols), BF16),
            pltpu.VMEM((tiles, channels * rows, LANES), F32),
            pltpu.VMEM((tiles, channels * rows, LANES), F32),
            pltpu.VMEM((tiles + 1, channels * rows // 2, LANES), F32),
            pltpu.VMEM((channels, 4 * rows, LANES), BF16),
            pltpu.VMEM((LANES, chan_up), F32),
            *[pltpu.VMEM((channels, LANES), F32)] * 4,
            pltpu.VMEM((rows, channels, cols), BF16),
            pltpu.VMEM((per, channels, lon_points), BF16),
            pltpu.VMEM((per, channels, lon_points), BF16),
            pltpu.VMEM((rows, channels, cols), BF16),
            *[pltpu.VMEM((channels, LANES), BF16)] * 6,
            *[pltpu.VMEM((HALO, channels, cols), BF16)] * 2,
            pltpu.VMEM((HALO, channels, lon_points), BF16),
            pltpu.VMEM(spec_gain.shape, F32),
            pltpu.VMEM((hid_up, channels), BF16),
            pltpu.VMEM((channels, hid_up), BF16),
            pltpu.VMEM((channels, channels), BF16),
            pltpu.VMEM((channels, LANES), F32),
            dma((len(operands),)),
            *[dma((2,))] * 6,
            *[dma((peers,))] * 2,
            *[dma((peers * per,))] * 4,
        ],
        compiler_params=pltpu.CompilerParams(
            collective_id=0, has_side_effects=True, vmem_limit_bytes=VMEM_LIMIT),
        name="block",
    )(*operands)


def solution(mesh):
    placed = (P(None, "lat", "lon"), P("lat", "lon"), P(), P(), P(), P(), P(), P(), P())
    return jax.shard_map(
        functools.partial(local, mesh.shape["lat"], mesh.shape["lon"]),
        mesh=mesh, in_specs=placed, out_specs=P(None, "lat", "lon"), check_vma=False,
    )
```

```python
import functools
import math

import jax
import jax.numpy as jnp
import numpy as np
from jax import lax
from jax.experimental import pallas as pl
from jax.experimental.pallas import tpu as pltpu
from jax.sharding import PartitionSpec as P

F32 = jnp.float32
BF16 = jnp.bfloat16
TAPS = 7
HALO = 3
LANES = 128
WORK = BF16
STEP = 30
VMEM_LIMIT = 58 * 1024 * 1024


def dft_table(lon_points, mode_count):
    phase = np.arange(lon_points)[:, None] * np.arange(mode_count)[None, :] % lon_points
    angles = phase.astype(np.float32) * np.float32(2.0 * math.pi / lon_points)
    factor = np.float32(1.0 / math.sqrt(lon_points))
    angles = angles.astype(np.float64)
    table = np.concatenate([np.cos(angles), -np.sin(angles)], axis=1).astype(np.float32)
    return (table * factor).astype(BF16)


def kernel(
    sizes,
    field_hbm, mask_hbm, fold_hbm, taps_hbm, gain_hbm, w_in_hbm, w_out_hbm, mix_hbm, spec_hbm, table_hbm,
    out_ref,
    field_ref, mask_ref, fold_ref, taps_ref, gain_ref, w_in_ref, w_out_ref, mix_ref, spec_raw, table_ref,
    flat, own, depth, flat_out, halo, toep, pattern_t, pattern, pattern_back, edge32, comb32,
    res, by_rows, back, spatial,
    edge_mine, edge_left, edge_right, comb, comb_n, comb_s, rows_n, rows_s, top_all,
    spec_ref, w_in_t, w_out_t, mix_t, gain_col,
    local_sem, edge_send, edge_recv, comb_send, comb_recv, rows_send, rows_recv,
    fold_send, fold_recv, out_send, out_recv, in_send, in_recv,
):
    channels, rows, cols, lat_n, lon_n, modes = sizes
    lon_points = cols * lon_n
    tiles = cols // LANES
    per = rows // lon_n
    step = max(u for u in range(2, STEP + 1, 2) if channels % u == 0)
    lat = lax.axis_index("lat")
    lon = lax.axis_index("lon")
    left = lax.rem(lon + lon_n - 1, lon_n)
    right = lax.rem(lon + 1, lon_n)
    chip = lon // 2
    core = lax.rem(lon, 2)
    chips = lon_n // 2
    mate_core = chip * 2 + 1 - core

    def target(k):
        return lax.rem(chip + k // 2, chips) * 2 + lax.rem(core + lax.rem(k, 2), 2)

    def source(k):
        return lax.rem(chip + chips - k // 2, chips) * 2 + lax.rem(core + lax.rem(k, 2), 2)

    whole = (
        (taps_hbm, taps_ref), (mask_hbm, mask_ref), (fold_hbm, fold_ref), (gain_hbm, gain_ref), (w_in_hbm, w_in_ref),
        (w_out_hbm, w_out_ref), (mix_hbm, mix_ref), (spec_hbm, spec_raw), (table_hbm, table_ref))
    loads = [pltpu.make_async_copy(a, b, local_sem.at[n]) for n, (a, b) in enumerate(whole)]
    groups = channels // step

    def field_load(group):
        some = pl.ds(group * step, step)
        return pltpu.make_async_copy(field_hbm.at[some], field_ref.at[some], local_sem.at[len(whole) + group])

    loads[0].start()
    loads[1].start()
    for group in range(groups):
        field_load(group).start()

    barrier = pltpu.get_barrier_semaphore()
    for k in range(1, lon_n):
        pl.semaphore_signal(barrier, inc=1, device_id={"lon": target(k)})

    @pl.when(lat > 0)
    def _():
        pl.semaphore_signal(barrier, inc=1, device_id={"lat": lat - 1})

    @pl.when(lat < lat_n - 1)
    def _():
        pl.semaphore_signal(barrier, inc=1, device_id={"lat": lat + 1})

    for load in loads[2:]:
        load.start()

    lane = lax.broadcasted_iota(jnp.int32, (rows, LANES), 1)
    loads[1].wait()
    wet = mask_ref[...].astype(F32)

    @pl.loop(0, channels // step)
    def _(group):
        for u in range(step):
            c = group * step + u
            if u == 0:
                field_load(group).wait()
            val = field_ref[c].astype(F32) * wet
            at = pl.multiple_of(c * rows, rows)
            parts = [val[:, h * LANES : (h + 1) * LANES] for h in range(tiles)]
            for h in range(tiles):
                flat[h, pl.ds(at, rows), :] = parts[h]
            edge = jnp.where(lane < HALO, parts[0], jnp.where(lane >= LANES - HALO, parts[-1], 0.0))
            edge = pltpu.roll(edge, 0, 1, stride=8, stride_axis=0)
            edge32[pl.ds(c, 1), :] = jnp.sum(edge, axis=0, keepdims=True)

    edge_mine[...] = edge32[...].astype(BF16)

    count = lon_n - 1 + jnp.where(lat > 0, 1, 0) + jnp.where(lat < lat_n - 1, 1, 0)
    pl.semaphore_wait(barrier, count)

    to_left = pltpu.make_async_remote_copy(
        edge_mine, edge_right, edge_send.at[0], edge_recv.at[0], device_id={"lon": left})
    to_right = pltpu.make_async_remote_copy(
        edge_mine, edge_left, edge_send.at[1], edge_recv.at[1], device_id={"lon": right})
    to_left.start()
    to_right.start()

    def own_row(i):
        for h in range(tiles):
            own[i, :, h * LANES : (h + 1) * LANES] = flat[h, pl.ds(i, channels, stride=rows), :].astype(BF16)

    rows_down = pltpu.make_async_remote_copy(
        own.at[pl.ds(0, HALO)], rows_n, rows_send.at[0], rows_recv.at[0], device_id={"lat": lat - 1})
    rows_up = pltpu.make_async_remote_copy(
        own.at[pl.ds(rows - HALO, HALO)], rows_s, rows_send.at[1], rows_recv.at[1], device_id={"lat": lat + 1})
    comb_down = pltpu.make_async_remote_copy(
        comb, comb_n, comb_send.at[0], comb_recv.at[0], device_id={"lat": lat - 1})
    comb_up = pltpu.make_async_remote_copy(
        comb, comb_s, comb_send.at[1], comb_recv.at[1], device_id={"lat": lat + 1})

    def piece(pos):
        return top_all.at[:, :, pl.ds(pl.multiple_of(pos * cols, LANES), cols)]

    def fold_out(j):
        whom = mate_core if j == 0 else lax.rem(chip + j, chips) * 2 + core
        return pltpu.make_async_remote_copy(
            own.at[pl.ds(rows - HALO, HALO)], piece(lon), fold_send.at[j], fold_recv.at[j], device_id={"lon": whom})

    def fold_pass(j):
        pos = lax.rem(chip + chips - j, chips) * 2 + core
        return pltpu.make_async_remote_copy(
            piece(pos), piece(pos), fold_send.at[chips + j - 1], fold_recv.at[chips + j - 1], device_id={"lon": mate_core})

    for i in range(rows - HALO, rows):
        own_row(i)

    @pl.when(lat < lat_n - 1)
    def _():
        rows_up.start()

    @pl.when(lat == lat_n - 1)
    def _():
        for j in range(chips - 1, -1, -1):
            fold_out(j).start()
        top_all[:, :, pl.ds(pl.multiple_of(lon * cols, LANES), cols)] = own[rows - HALO :]

    for i in range(HALO):
        own_row(i)

    @pl.when(lat > 0)
    def _():
        rows_down.start()

    loads[0].wait()
    pattern_t[...] = jnp.zeros(pattern_t.shape, F32)
    for a in range(TAPS):
        for b in range(TAPS):
            pattern_t[b * rows + a : b * rows + a + 1, :channels] = taps_ref[a, b : b + 1, :]
    pattern[...] = pattern_t[...].T[:channels]
    pattern_back[...] = pltpu.roll(pattern[...], LANES - HALO, 1)

    slot = lax.rem(lane, rows)
    index = lax.broadcasted_iota(jnp.int32, (rows, LANES), 0)
    band = jnp.abs(slot - index) <= HALO
    half = rows // 2
    low_slot = slot[:half] < HALO
    high_slot = (slot[:half] >= half + HALO) & (slot[:half] < half + 2 * HALO)

    @pl.loop(0, channels // step)
    def _(group):
        for u in range(step):
            c = group * step + u
            row = jnp.broadcast_to(pattern_back[pl.ds(c, 1), :], (rows, LANES))
            mid = jnp.where(band, pltpu.roll(row, 0, 1, stride=1, stride_axis=0), 0.0)
            row = jnp.broadcast_to(pattern[pl.ds(c, 1), :], (half, LANES))
            far = pltpu.roll(row, 0, 1, stride=1, stride_axis=0)
            far = jnp.concatenate([jnp.where(low_slot, far, 0.0), jnp.where(high_slot, far, 0.0)], axis=0)
            for n, part in enumerate((mid, far)):
                coarse = part.astype(BF16)
                toep[c, 2 * n * rows : (2 * n + 1) * rows, :] = coarse
                toep[c, (2 * n + 1) * rows : (2 * n + 2) * rows, :] = (part - coarse.astype(F32)).astype(BF16)

    halo[...] = jnp.zeros(halo.shape, F32)

    def turned(ref, target_ref):
        n, m = ref.shape
        up = [-(-d // LANES) * LANES for d in (n, m)]
        full = jnp.concatenate([ref[...].astype(F32), jnp.zeros((n, up[1] - m), F32)], axis=1)
        full = jnp.concatenate([full, jnp.zeros((up[0] - n, up[1]), F32)], axis=0)
        target_ref[...] = full.T[: target_ref.shape[0], : target_ref.shape[1]].astype(BF16)

    for n in range(3, 7):
        loads[n].wait()
    turned(w_in_ref, w_in_t)
    w_out_t[...] = jnp.zeros(w_out_t.shape, BF16)
    w_out_t[:, : w_out_ref.shape[1]] = w_out_ref[...]
    turned(mix_ref, mix_t)
    diagonal = lax.broadcasted_iota(jnp.int32, (channels, channels), 0) == lax.broadcasted_iota(
        jnp.int32, (channels, channels), 1)
    gain_col[...] = jnp.broadcast_to(
        jnp.sum(jnp.where(diagonal, gain_ref[...], 0.0), axis=1, keepdims=True), (channels, LANES))

    for i in range(HALO, rows - HALO):
        own_row(i)

    to_left.wait()
    to_right.wait()
    near = lax.rem(lax.broadcasted_iota(jnp.int32, (channels, LANES), 1), 8) < 4
    both = jnp.where(near, edge_right[...].astype(F32), edge_left[...].astype(F32))
    comb[...] = both.astype(BF16)
    comb32[...] = both

    @pl.when(lat > 0)
    def _():
        comb_down.start()

    @pl.when(lat < lat_n - 1)
    def _():
        comb_up.start()

    def shifted(ring, finish_block):
        high = ring[0].shape[0]
        at = lane[:high]
        blocks = []
        for b in range(TAPS):
            d = b - HALO
            line = []
            for h in range(tiles):
                if d == 0:
                    line.append(ring[h])
                elif d > 0:
                    line.append(pltpu.roll(jnp.where(at < d, ring[h + 1], ring[h]), LANES - d, 1))
                else:
                    line.append(pltpu.roll(jnp.where(at >= LANES + d, ring[h - 1], ring[h]), -d, 1))
            blocks.append(finish_block(jnp.concatenate(line, axis=1)))
        return jnp.concatenate(blocks + [blocks[-1]] * (LANES // rows - TAPS), axis=0)

    blank = jnp.zeros((2 * rows, LANES), BF16)

    def product(c, which, rings, finish_block):
        span = slice(2 * which * rows, 2 * (which + 1) * rows)
        weights = jnp.concatenate(
            [jnp.concatenate([toep[c, span, :], blank], axis=1), jnp.concatenate([blank, toep[c + 1, span, :]], axis=1)],
            axis=0)
        points = jnp.concatenate([shifted(ring, finish_block) for ring in rings], axis=0)
        total = jnp.dot(weights, points, preferred_element_type=F32)
        return total[:rows] + total[rows : 2 * rows], total[2 * rows : 3 * rows] + total[3 * rows :]

    @pl.loop(0, channels // step)
    def _(group):
        for u in range(0, step, 2):
            rings = []
            for c in (group * step + u, group * step + u + 1):
                rim = jnp.broadcast_to(comb32[pl.ds(c, 1), :], (half, LANES))
                for bit in (1, 2, 4):
                    rim = jnp.where(lax.rem(index[:half] // bit, 2) == 1, pltpu.roll(rim, LANES - 8 * bit, 1), rim)
                rim = jnp.concatenate([rim, pltpu.roll(rim, LANES - 8 * half, 1)], axis=0)
                at = pl.multiple_of(c * rows, rows)
                rings.append([flat[h, pl.ds(at, rows), :].astype(WORK) for h in range(tiles)] + [rim.astype(WORK)])
            totals = product(group * step + u, 0, rings, lambda block: block.astype(BF16))
            for n, total in enumerate(totals):
                at = pl.multiple_of((group * step + u + n) * rows, rows)
                for h in range(tiles):
                    depth[h, pl.ds(at, rows), :] = total[:, h * LANES : (h + 1) * LANES]

    def edges_of(packed, i):
        return pltpu.roll(packed, LANES - 8 * i, 1) if i else packed

    def put_halo(at, value, rim):
        for h in range(tiles):
            halo[h, pl.ds(at, channels, stride=half), :] = value[:, h * LANES : (h + 1) * LANES]
        halo[tiles, pl.ds(at, channels, stride=half), :] = rim

    def await_halo():
        loads[2].wait()

        @pl.when(lat > 0)
        def _():
            rows_down.wait_send()
            comb_down.wait_send()
            rows_up.wait_recv()
            comb_up.wait_recv()
            for r in range(HALO):
                put_halo(r, rows_s[r].astype(F32), edges_of(comb_s[...].astype(F32), rows - HALO + r))

        @pl.when(lat < lat_n - 1)
        def _():
            rows_up.wait_send()
            comb_up.wait_send()
            rows_down.wait_recv()
            comb_down.wait_recv()
            for r in range(HALO):
                put_halo(HALO + r, rows_n[r].astype(F32), edges_of(comb_n[...].astype(F32), r))

        @pl.when(lat == lat_n - 1)
        def _():
            for j in range(1, chips):
                fold_out(j).wait_recv()
                fold_pass(j).start()
            for j in range(chips):
                fold_out(j).wait_send()
            fold_out(0).wait_recv()
            for j in range(1, chips):
                fold_pass(j).wait()
            point = lax.broadcasted_iota(jnp.int32, (lon_points, cols + LANES), 0)
            at = lax.broadcasted_iota(jnp.int32, (1, cols + LANES), 1)
            at = jnp.where(at < cols + HALO, at, at - (cols + LANES)) + lon * cols
            mate = fold_ref[:, :1] - at
            mate = jnp.where(mate < 0, mate + lon_points, mate)
            mate = jnp.where(mate < 0, mate + lon_points, mate)
            mate = jnp.where(mate >= lon_points, mate - lon_points, mate)
            pick = jnp.where(point == mate, 1.0, 0.0).astype(BF16)
            for r in range(HALO):
                row = jnp.dot(top_all[HALO - 1 - r], pick, preferred_element_type=F32)
                put_halo(HALO + r, row[:, :cols], row[:, cols:])

        @pl.loop(0, channels // step)
        def _(group):
            for u in range(0, step, 2):
                rings = []
                for c in (group * step + u, group * step + u + 1):
                    spot = pl.ds(pl.multiple_of(c * half, half), half)
                    rings.append([halo[h, spot, :] for h in range(tiles + 1)])
                totals = product(
                    group * step + u, 1, rings, lambda block: jnp.concatenate([block, block], axis=0).astype(BF16))
                for n, total in enumerate(totals):
                    at = pl.multiple_of((group * step + u + n) * rows, rows)
                    for h in range(tiles):
                        depth[h, pl.ds(at, rows), :] += total[:, h * LANES : (h + 1) * LANES]

    here = pl.ds(pl.multiple_of(lon * cols, LANES), cols)

    def row_at(chunk, q):
        return lax.rem(chunk * lon_n + q + HALO, rows)

    def send_row(chunk, k):
        s = chunk * (lon_n - 1) + lon_n - 1 - k
        return pltpu.make_async_remote_copy(
            res.at[row_at(chunk, target(k))], by_rows.at[chunk, :, here],
            out_send.at[s], out_recv.at[s], device_id={"lon": target(k)})

    def send_back(chunk, k):
        q = target(k)
        s = chunk * (lon_n - 1) + lon_n - 1 - k
        return pltpu.make_async_remote_copy(
            back.at[chunk, :, pl.ds(pl.multiple_of(q * cols, LANES), cols)], spatial.at[chunk * lon_n + lon],
            in_send.at[s], in_recv.at[s], device_id={"lon": q})

    def mix_rows(first, last):
        @pl.loop(first * (lon_n // 2), last * (lon_n // 2))
        def _(at):
            chunk = at // (lon_n // 2)
            pair = lax.rem(at, lon_n // 2)
            k = lon_n - 1 - 2 * pair
            one, two = row_at(chunk, target(k)), row_at(chunk, target(k - 1))
            x = jnp.concatenate(
                [depth[h, pl.ds(row, channels, stride=rows), :] for row in (one, two) for h in range(tiles)], axis=1)
            mean = jnp.sum(x, axis=0, keepdims=True) * (1.0 / channels)
            centred = x - mean
            var = jnp.sum(centred * centred, axis=0, keepdims=True) * (1.0 / channels)
            gain = jnp.concatenate([gain_col[...]] * (2 * tiles), axis=1)
            normed = (centred * lax.rsqrt(var + 1e-06) * gain).astype(BF16)
            pre = jnp.dot(w_in_t[...], normed, preferred_element_type=F32)
            hidden = jax.nn.gelu(pre, approximate=True).astype(BF16)
            branch = jnp.dot(w_out_t[...], hidden, preferred_element_type=F32)
            for n, row in enumerate((one, two)):
                wet_row = mask_ref[pl.ds(row, 1), :].astype(F32)
                part = branch[:, n * cols : (n + 1) * cols]
                res[row] = (wet_row * (own[row].astype(F32) + part)).astype(BF16)
            send_row(chunk, k).start()

            @pl.when(pair < lon_n // 2 - 1)
            def _():
                send_row(chunk, k - 1).start()

            @pl.when(pair == lon_n // 2 - 1)
            def _():
                by_rows[chunk, :, here] = res[two]

    def spectral(chunk):
        for k in range(lon_n - 1, 0, -1):
            send_row(chunk, k).wait_recv()
        spectrum = jnp.dot(by_rows[chunk], table_ref[...], preferred_element_type=F32)
        s_re = spectrum[:, :modes]
        s_im = spectrum[:, modes:]
        g_re = spec_ref[0]
        g_im = spec_ref[1]
        scaled = jnp.concatenate(
            [(g_re * s_re - g_im * s_im).astype(BF16), (g_re * s_im + g_im * s_re).astype(BF16)], axis=1)
        back[chunk] = lax.dot_general(
            scaled, table_ref[...], (((1,), (1,)), ((), ())), preferred_element_type=F32).astype(BF16)
        for k in range(lon_n - 1, 0, -1):
            send_back(chunk, k).start()
        spatial[chunk * lon_n + lon] = back[chunk, :, here]

    def finish(chunk):
        @pl.loop(0, lon_n // 2)
        def _(pair):
            k = 2 * pair

            @pl.when(pair > 0)
            def _():
                send_back(chunk, k).wait_recv()

            send_back(chunk, k + 1).wait_recv()
            spots = [source(k), source(k + 1)]
            points = jnp.concatenate([spatial[chunk * lon_n + pos] for pos in spots], axis=1)
            mixed = jnp.dot(mix_t[...], points, preferred_element_type=F32)
            for n, pos in enumerate(spots):
                row = row_at(chunk, pos)
                wet_row = mask_ref[pl.ds(row, 1), :].astype(F32)
                val = wet_row * (res[row].astype(F32) + mixed[:, n * cols : (n + 1) * cols])
                for h in range(tiles):
                    flat_out[h, pl.ds(row, channels, stride=rows), :] = val[:, h * LANES : (h + 1) * LANES]

    needs = [
        any((chunk * lon_n + q + HALO) % rows < HALO or (chunk * lon_n + q + HALO) % rows >= rows - HALO for q in range(lon_n))
        for chunk in range(per)]
    early = needs.index(True)
    if early:
        mix_rows(0, early)
    loads[7].wait()
    wide = modes // LANES
    for p in range(2):
        for t in range(wide):
            spec_ref[p, :, t * LANES : (t + 1) * LANES] = spec_raw[pl.ds(2 * t + p, channels, stride=2 * wide), :]
    loads[8].wait()
    if early:
        pl.loop(0, early)(spectral)
    await_halo()
    mix_rows(early, per)
    pl.loop(early, per)(spectral)
    pl.loop(0, per)(finish)

    @pl.loop(0, channels // step)
    def _(group):
        for u in range(step):
            c = group * step + u
            at = pl.multiple_of(c * rows, rows)
            for h in range(tiles):
                out_ref[c, :, h * LANES : (h + 1) * LANES] = flat_out[h, pl.ds(at, rows), :].astype(BF16)

    for chunk in range(per):
        for k in range(lon_n - 1, 0, -1):
            send_row(chunk, k).wait_send()
            send_back(chunk, k).wait_send()


def local(lat_n, lon_n, field, land_mask, fold_partner, dw_kernel, norm_gain, w_in, w_out, spec_gain, mix_weight):
    channels, rows, cols = field.shape
    modes = spec_gain.shape[2]
    hid = w_in.shape[1]
    lon_points = cols * lon_n
    hid_up = -(-hid // 16) * 16
    chan_up = -(-channels // LANES) * LANES
    tiles = cols // LANES
    table = jnp.asarray(dft_table(lon_points, modes))
    taps = dw_kernel.transpose(1, 2, 0)
    wide = modes // LANES
    spec = spec_gain.transpose(1, 0, 2).reshape(channels, 2, wide, LANES).transpose(0, 2, 1, 3).reshape(-1, LANES)
    per = rows // lon_n
    sizes = (channels, rows, cols, lat_n, lon_n, modes)
    operands = (field, land_mask, fold_partner[None, :], taps, norm_gain[None, :], w_in, w_out.T, mix_weight, spec, table)
    dma = pltpu.SemaphoreType.DMA
    peers = lon_n - 1
    return pl.pallas_call(
        functools.partial(kernel, sizes),
        out_shape=pltpu.VMEM(field.shape, BF16),
        in_specs=[pl.BlockSpec(memory_space=pltpu.HBM)] * len(operands),
        out_specs=pl.BlockSpec(memory_space=pltpu.VMEM),
        scratch_shapes=[
            *[pltpu.VMEM(x.shape, x.dtype) for x in operands],
            pltpu.VMEM((tiles, channels * rows, LANES), F32),
            pltpu.VMEM((rows, channels, cols), BF16),
            pltpu.VMEM((tiles, channels * rows, LANES), F32),
            pltpu.VMEM((tiles, channels * rows, LANES), F32),
            pltpu.VMEM((tiles + 1, channels * rows // 2, LANES), F32),
            pltpu.VMEM((channels, 4 * rows, LANES), BF16),
            pltpu.VMEM((LANES, chan_up), F32),
            *[pltpu.VMEM((channels, LANES), F32)] * 4,
            pltpu.VMEM((rows, channels, cols), BF16),
            pltpu.VMEM((per, channels, lon_points), BF16),
            pltpu.VMEM((per, channels, lon_points), BF16),
            pltpu.VMEM((rows, channels, cols), BF16),
            *[pltpu.VMEM((channels, LANES), BF16)] * 6,
            *[pltpu.VMEM((HALO, channels, cols), BF16)] * 2,
            pltpu.VMEM((HALO, channels, lon_points), BF16),
            pltpu.VMEM(spec_gain.shape, F32),
            pltpu.VMEM((hid_up, channels), BF16),
            pltpu.VMEM((channels, hid_up), BF16),
            pltpu.VMEM((channels, channels), BF16),
            pltpu.VMEM((channels, LANES), F32),
            dma((2 * len(operands) + channels,)),
            *[dma((2,))] * 6,
            *[dma((peers,))] * 2,
            *[dma((peers * per,))] * 4,
        ],
        compiler_params=pltpu.CompilerParams(
            collective_id=0, has_side_effects=True, vmem_limit_bytes=VMEM_LIMIT),
        name="block",
    )(*operands)


def solution(mesh):
    placed = (P(None, "lat", "lon"), P("lat", "lon"), P(), P(), P(), P(), P(), P(), P())
    return jax.shard_map(
        functools.partial(local, mesh.shape["lat"], mesh.shape["lon"]),
        mesh=mesh, in_specs=placed, out_specs=P(None, "lat", "lon"), check_vma=False,
    )
```

```python
import functools
import math

import jax
import jax.numpy as jnp
import numpy as np
from jax import lax
from jax.experimental import pallas as pl
from jax.experimental.pallas import tpu as pltpu
from jax.sharding import PartitionSpec as P

F32 = jnp.float32
BF16 = jnp.bfloat16
TAPS = 7
HALO = 3
LANES = 128
WORK = BF16
GELU_LINE = math.sqrt(2.0 / math.pi)
GELU_CUBE = 0.044715 * GELU_LINE
STEP = 30
VMEM_LIMIT = 58 * 1024 * 1024


def dft_table(lon_points, mode_count):
    phase = np.arange(lon_points)[:, None] * np.arange(mode_count)[None, :] % lon_points
    angles = phase.astype(np.float32) * np.float32(2.0 * math.pi / lon_points)
    factor = np.float32(1.0 / math.sqrt(lon_points))
    angles = angles.astype(np.float64)
    table = np.concatenate([np.cos(angles), -np.sin(angles)], axis=1).astype(np.float32)
    return (table * factor).astype(BF16)


def kernel(
    sizes,
    field_hbm, mask_hbm, fold_hbm, taps_hbm, gain_hbm, w_in_hbm, w_out_hbm, mix_hbm, spec_hbm, table_hbm,
    out_ref,
    field_ref, mask_ref, fold_ref, taps_ref, gain_ref, w_in_ref, w_out_ref, mix_ref, spec_raw, table_ref,
    flat, own, depth, flat_out, halo, toep, pattern_t, pattern, pattern_back, edge32, comb32,
    res, by_rows, back, spatial,
    edge_mine, edge_left, edge_right, comb, comb_n, comb_s, rows_n, rows_s, top_all,
    spec_ref, w_in_t, w_out_t, mix_t, gain_col,
    local_sem, edge_send, edge_recv, comb_send, comb_recv, rows_send, rows_recv,
    fold_send, fold_recv, out_send, out_recv, in_send, in_recv,
):
    channels, rows, cols, lat_n, lon_n, modes = sizes
    lon_points = cols * lon_n
    tiles = cols // LANES
    per = rows // lon_n
    step = max(u for u in range(2, STEP + 1, 2) if channels % u == 0)
    lat = lax.axis_index("lat")
    lon = lax.axis_index("lon")
    left = lax.rem(lon + lon_n - 1, lon_n)
    right = lax.rem(lon + 1, lon_n)
    chip = lon // 2
    core = lax.rem(lon, 2)
    chips = lon_n // 2
    mate_core = chip * 2 + 1 - core

    def target(k):
        return lax.rem(chip + k // 2, chips) * 2 + lax.rem(core + lax.rem(k, 2), 2)

    def source(k):
        return lax.rem(chip + chips - k // 2, chips) * 2 + lax.rem(core + lax.rem(k, 2), 2)

    whole = (
        (taps_hbm, taps_ref), (mask_hbm, mask_ref), (fold_hbm, fold_ref), (gain_hbm, gain_ref), (w_in_hbm, w_in_ref),
        (w_out_hbm, w_out_ref), (mix_hbm, mix_ref), (spec_hbm, spec_raw), (table_hbm, table_ref))
    loads = [pltpu.make_async_copy(a, b, local_sem.at[n]) for n, (a, b) in enumerate(whole)]
    groups = channels // step

    def field_load(group):
        some = pl.ds(group * step, step)
        return pltpu.make_async_copy(field_hbm.at[some], field_ref.at[some], local_sem.at[len(whole) + group])

    loads[0].start()
    loads[1].start()
    for group in range(groups):
        field_load(group).start()

    barrier = pltpu.get_barrier_semaphore()
    for k in range(1, lon_n):
        pl.semaphore_signal(barrier, inc=1, device_id={"lon": target(k)})

    @pl.when(lat > 0)
    def _():
        pl.semaphore_signal(barrier, inc=1, device_id={"lat": lat - 1})

    @pl.when(lat < lat_n - 1)
    def _():
        pl.semaphore_signal(barrier, inc=1, device_id={"lat": lat + 1})

    lane = lax.broadcasted_iota(jnp.int32, (rows, LANES), 1)
    half = rows // 2
    loads[1].wait()
    wet = mask_ref[...].astype(F32)

    @pl.loop(0, channels // step)
    def _(group):
        for u in range(step):
            c = group * step + u
            if u == 0:
                field_load(group).wait()
            val = field_ref[c].astype(F32) * wet
            at = pl.multiple_of(c * rows, rows)
            parts = [val[:, h * LANES : (h + 1) * LANES] for h in range(tiles)]
            for h in range(tiles):
                flat[h, pl.ds(at, rows), :] = parts[h]
            edge = jnp.where(lane < HALO, parts[0], jnp.where(lane >= LANES - HALO, parts[-1], 0.0))
            edge = edge[:half] + pltpu.roll(edge[half:], LANES - 8 * half, 1)
            for hop in (4, 2, 1):
                edge = edge + pltpu.roll(pltpu.roll(edge, half - hop, 0), LANES - 8 * hop, 1)
            edge32[pl.ds(c, 1), :] = edge[:1]

    for load in loads[2:]:
        load.start()

    edge_mine[...] = edge32[...].astype(BF16)

    count = lon_n - 1 + jnp.where(lat > 0, 1, 0) + jnp.where(lat < lat_n - 1, 1, 0)
    pl.semaphore_wait(barrier, count)

    to_left = pltpu.make_async_remote_copy(
        edge_mine, edge_right, edge_send.at[0], edge_recv.at[0], device_id={"lon": left})
    to_right = pltpu.make_async_remote_copy(
        edge_mine, edge_left, edge_send.at[1], edge_recv.at[1], device_id={"lon": right})
    to_left.start()
    to_right.start()

    def own_row(i):
        for h in range(tiles):
            own[i, :, h * LANES : (h + 1) * LANES] = flat[h, pl.ds(i, channels, stride=rows), :].astype(BF16)

    rows_down = pltpu.make_async_remote_copy(
        own.at[pl.ds(0, HALO)], rows_n, rows_send.at[0], rows_recv.at[0], device_id={"lat": lat - 1})
    rows_up = pltpu.make_async_remote_copy(
        own.at[pl.ds(rows - HALO, HALO)], rows_s, rows_send.at[1], rows_recv.at[1], device_id={"lat": lat + 1})
    comb_down = pltpu.make_async_remote_copy(
        comb, comb_n, comb_send.at[0], comb_recv.at[0], device_id={"lat": lat - 1})
    comb_up = pltpu.make_async_remote_copy(
        comb, comb_s, comb_send.at[1], comb_recv.at[1], device_id={"lat": lat + 1})

    def piece(pos):
        return top_all.at[:, :, pl.ds(pl.multiple_of(pos * cols, LANES), cols)]

    def fold_out(j):
        whom = mate_core if j == 0 else lax.rem(chip + j, chips) * 2 + core
        return pltpu.make_async_remote_copy(
            own.at[pl.ds(rows - HALO, HALO)], piece(lon), fold_send.at[j], fold_recv.at[j], device_id={"lon": whom})

    def fold_pass(j):
        pos = lax.rem(chip + chips - j, chips) * 2 + core
        return pltpu.make_async_remote_copy(
            piece(pos), piece(pos), fold_send.at[chips + j - 1], fold_recv.at[chips + j - 1], device_id={"lon": mate_core})

    for i in range(rows - HALO, rows):
        own_row(i)

    @pl.when(lat < lat_n - 1)
    def _():
        rows_up.start()

    @pl.when(lat == lat_n - 1)
    def _():
        for j in range(chips - 1, -1, -1):
            fold_out(j).start()
        top_all[:, :, pl.ds(pl.multiple_of(lon * cols, LANES), cols)] = own[rows - HALO :]

    for i in range(HALO):
        own_row(i)

    @pl.when(lat > 0)
    def _():
        rows_down.start()

    loads[0].wait()
    pattern_t[...] = jnp.zeros(pattern_t.shape, F32)
    for a in range(TAPS):
        for b in range(TAPS):
            pattern_t[b * rows + a : b * rows + a + 1, :channels] = taps_ref[a, b : b + 1, :]
    pattern[...] = pattern_t[...].T[:channels]
    pattern_back[...] = pltpu.roll(pattern[...], LANES - HALO, 1)

    slot = lax.rem(lane, rows)
    index = lax.broadcasted_iota(jnp.int32, (rows, LANES), 0)
    band = jnp.abs(slot - index) <= HALO
    low_slot = slot[:half] < HALO
    high_slot = (slot[:half] >= half + HALO) & (slot[:half] < half + 2 * HALO)

    @pl.loop(0, channels // step)
    def _(group):
        for u in range(step):
            c = group * step + u
            row = jnp.broadcast_to(pattern_back[pl.ds(c, 1), :], (rows, LANES))
            mid = jnp.where(band, pltpu.roll(row, 0, 1, stride=1, stride_axis=0), 0.0)
            row = jnp.broadcast_to(pattern[pl.ds(c, 1), :], (half, LANES))
            far = pltpu.roll(row, 0, 1, stride=1, stride_axis=0)
            far = jnp.concatenate([jnp.where(low_slot, far, 0.0), jnp.where(high_slot, far, 0.0)], axis=0)
            for n, part in enumerate((mid, far)):
                coarse = part.astype(BF16)
                toep[c, 2 * n * rows : (2 * n + 1) * rows, :] = coarse
                toep[c, (2 * n + 1) * rows : (2 * n + 2) * rows, :] = (part - coarse.astype(F32)).astype(BF16)

    halo[...] = jnp.zeros(halo.shape, F32)

    def turned(ref, target_ref):
        n, m = ref.shape
        up = [-(-d // LANES) * LANES for d in (n, m)]
        full = jnp.concatenate([ref[...].astype(F32), jnp.zeros((n, up[1] - m), F32)], axis=1)
        full = jnp.concatenate([full, jnp.zeros((up[0] - n, up[1]), F32)], axis=0)
        target_ref[...] = full.T[: target_ref.shape[0], : target_ref.shape[1]].astype(BF16)

    for n in range(3, 7):
        loads[n].wait()
    turned(w_in_ref, w_in_t)
    w_out_t[...] = jnp.zeros(w_out_t.shape, BF16)
    w_out_t[:, : w_out_ref.shape[1]] = w_out_ref[...]
    turned(mix_ref, mix_t)
    diagonal = lax.broadcasted_iota(jnp.int32, (channels, channels), 0) == lax.broadcasted_iota(
        jnp.int32, (channels, channels), 1)
    gain_col[...] = jnp.broadcast_to(
        jnp.sum(jnp.where(diagonal, gain_ref[...], 0.0), axis=1, keepdims=True), (channels, LANES))

    for i in range(HALO, rows - HALO):
        own_row(i)

    to_left.wait()
    to_right.wait()
    near = lax.rem(lax.broadcasted_iota(jnp.int32, (channels, LANES), 1), 8) < 4
    both = jnp.where(near, edge_right[...].astype(F32), edge_left[...].astype(F32))
    comb[...] = both.astype(BF16)
    comb32[...] = both

    @pl.when(lat > 0)
    def _():
        comb_down.start()

    @pl.when(lat < lat_n - 1)
    def _():
        comb_up.start()

    def shifted(ring, finish_block):
        high = ring[0].shape[0]
        at = lane[:high]
        blocks = []
        for b in range(TAPS):
            d = b - HALO
            line = []
            for h in range(tiles):
                if d == 0:
                    line.append(ring[h])
                elif d > 0:
                    line.append(pltpu.roll(jnp.where(at < d, ring[h + 1], ring[h]), LANES - d, 1))
                else:
                    line.append(pltpu.roll(jnp.where(at >= LANES + d, ring[h - 1], ring[h]), -d, 1))
            blocks.append(finish_block(jnp.concatenate(line, axis=1)))
        return jnp.concatenate(blocks + [blocks[-1]] * (LANES // rows - TAPS), axis=0)

    blank = jnp.zeros((2 * rows, LANES), BF16)

    def product(c, which, rings, finish_block):
        span = slice(2 * which * rows, 2 * (which + 1) * rows)
        weights = jnp.concatenate(
            [jnp.concatenate([toep[c, span, :], blank], axis=1), jnp.concatenate([blank, toep[c + 1, span, :]], axis=1)],
            axis=0)
        points = jnp.concatenate([shifted(ring, finish_block) for ring in rings], axis=0)
        total = jnp.dot(weights, points, preferred_element_type=F32)
        return total[:rows] + total[rows : 2 * rows], total[2 * rows : 3 * rows] + total[3 * rows :]

    @pl.loop(0, channels // step)
    def _(group):
        for u in range(0, step, 2):
            rings = []
            for c in (group * step + u, group * step + u + 1):
                rim = jnp.broadcast_to(comb32[pl.ds(c, 1), :], (rows, LANES))
                rim = pltpu.roll(rim, 0, 1, stride=8, stride_axis=0)
                at = pl.multiple_of(c * rows, rows)
                rings.append([flat[h, pl.ds(at, rows), :].astype(WORK) for h in range(tiles)] + [rim.astype(WORK)])
            totals = product(group * step + u, 0, rings, lambda block: block.astype(BF16))
            for n, total in enumerate(totals):
                at = pl.multiple_of((group * step + u + n) * rows, rows)
                for h in range(tiles):
                    depth[h, pl.ds(at, rows), :] = total[:, h * LANES : (h + 1) * LANES]

    def edges_of(packed, i):
        return pltpu.roll(packed, 8 * i, 1) if i else packed

    def put_halo(at, value, rim):
        for h in range(tiles):
            halo[h, pl.ds(at, channels, stride=half), :] = value[:, h * LANES : (h + 1) * LANES]
        halo[tiles, pl.ds(at, channels, stride=half), :] = rim

    def await_halo():
        loads[2].wait()

        @pl.when(lat > 0)
        def _():
            rows_down.wait_send()
            comb_down.wait_send()
            rows_up.wait_recv()
            comb_up.wait_recv()
            for r in range(HALO):
                put_halo(r, rows_s[r].astype(F32), edges_of(comb_s[...].astype(F32), rows - HALO + r))

        @pl.when(lat < lat_n - 1)
        def _():
            rows_up.wait_send()
            comb_up.wait_send()
            rows_down.wait_recv()
            comb_down.wait_recv()
            for r in range(HALO):
                put_halo(HALO + r, rows_n[r].astype(F32), edges_of(comb_n[...].astype(F32), r))

        @pl.when(lat == lat_n - 1)
        def _():
            for j in range(1, chips):
                fold_out(j).wait_recv()
                fold_pass(j).start()
            for j in range(chips):
                fold_out(j).wait_send()
            fold_out(0).wait_recv()
            for j in range(1, chips):
                fold_pass(j).wait()
            point = lax.broadcasted_iota(jnp.int32, (lon_points, cols + LANES), 0)
            at = lax.broadcasted_iota(jnp.int32, (1, cols + LANES), 1)
            at = jnp.where(at < cols + HALO, at, at - (cols + LANES)) + lon * cols
            mate = fold_ref[:, :1] - at
            mate = jnp.where(mate < 0, mate + lon_points, mate)
            mate = jnp.where(mate < 0, mate + lon_points, mate)
            mate = jnp.where(mate >= lon_points, mate - lon_points, mate)
            pick = jnp.where(point == mate, 1.0, 0.0).astype(BF16)
            for r in range(HALO):
                row = jnp.dot(top_all[HALO - 1 - r], pick, preferred_element_type=F32)
                put_halo(HALO + r, row[:, :cols], row[:, cols:])

    def halo_conv():
        @pl.loop(0, channels // step)
        def _(group):
            for u in range(0, step, 2):
                rings = []
                for c in (group * step + u, group * step + u + 1):
                    spot = pl.ds(pl.multiple_of(c * half, half), half)
                    rings.append([halo[h, spot, :] for h in range(tiles + 1)])
                totals = product(
                    group * step + u, 1, rings, lambda block: jnp.concatenate([block, block], axis=0).astype(BF16))
                for n, total in enumerate(totals):
                    at = pl.multiple_of((group * step + u + n) * rows, rows)
                    for h in range(tiles):
                        depth[h, pl.ds(at, rows), :] += total[:, h * LANES : (h + 1) * LANES]

    here = pl.ds(pl.multiple_of(lon * cols, LANES), cols)

    def row_at(chunk, q):
        return lax.rem(chunk * lon_n + q + HALO, rows)

    def send_row(chunk, k):
        s = chunk * (lon_n - 1) + lon_n - 1 - k
        return pltpu.make_async_remote_copy(
            res.at[row_at(chunk, target(k))], by_rows.at[chunk, :, here],
            out_send.at[s], out_recv.at[s], device_id={"lon": target(k)})

    def send_back(chunk, k):
        q = target(k)
        s = chunk * (lon_n - 1) + lon_n - 1 - k
        return pltpu.make_async_remote_copy(
            back.at[chunk, :, pl.ds(pl.multiple_of(q * cols, LANES), cols)], spatial.at[chunk * lon_n + lon],
            in_send.at[s], in_recv.at[s], device_id={"lon": q})

    def mix_rows(first, last):
        @pl.loop(first * (lon_n // 2), last * (lon_n // 2))
        def _(at):
            chunk = at // (lon_n // 2)
            pair = lax.rem(at, lon_n // 2)
            k = lon_n - 1 - 2 * pair
            one, two = row_at(chunk, target(k)), row_at(chunk, target(k - 1))
            x = jnp.concatenate(
                [depth[h, pl.ds(row, channels, stride=rows), :] for row in (one, two) for h in range(tiles)], axis=1)
            mean = jnp.sum(x, axis=0, keepdims=True) * (1.0 / channels)
            centred = x - mean
            var = jnp.sum(centred * centred, axis=0, keepdims=True) * (1.0 / channels)
            gain = jnp.concatenate([gain_col[...]] * (2 * tiles), axis=1)
            normed = (centred * lax.rsqrt(var + 1e-06) * gain).astype(BF16)
            pre = jnp.dot(w_in_t[...], normed, preferred_element_type=F32)
            inner = pre * (GELU_CUBE * (pre * pre) + GELU_LINE)
            hidden = (pre + pre * jnp.tanh(inner)).astype(BF16)
            branch = jnp.dot(w_out_t[...], hidden, preferred_element_type=F32)
            for n, row in enumerate((one, two)):
                wet_row = mask_ref[pl.ds(row, 1), :].astype(F32)
                part = 0.5 * branch[:, n * cols : (n + 1) * cols]
                res[row] = (wet_row * (own[row].astype(F32) + part)).astype(BF16)
            send_row(chunk, k).start()

            @pl.when(pair < lon_n // 2 - 1)
            def _():
                send_row(chunk, k - 1).start()

            @pl.when(pair == lon_n // 2 - 1)
            def _():
                by_rows[chunk, :, here] = res[two]

    def spectral(chunk):
        for k in range(lon_n - 1, 0, -1):
            send_row(chunk, k).wait_recv()
        spectrum = jnp.dot(by_rows[chunk], table_ref[...], preferred_element_type=F32)
        s_re = spectrum[:, :modes]
        s_im = spectrum[:, modes:]
        g_re = spec_ref[0]
        g_im = spec_ref[1]
        scaled = jnp.concatenate(
            [(g_re * s_re - g_im * s_im).astype(BF16), (g_re * s_im + g_im * s_re).astype(BF16)], axis=1)
        back[chunk] = lax.dot_general(
            scaled, table_ref[...], (((1,), (1,)), ((), ())), preferred_element_type=F32).astype(BF16)
        for k in range(lon_n - 1, 0, -1):
            send_back(chunk, k).start()
        spatial[chunk * lon_n + lon] = back[chunk, :, here]

    def finish(chunk):
        @pl.loop(0, lon_n // 2)
        def _(pair):
            k = 2 * pair

            @pl.when(pair > 0)
            def _():
                send_back(chunk, k).wait_recv()

            send_back(chunk, k + 1).wait_recv()
            spots = [source(k), source(k + 1)]
            points = jnp.concatenate([spatial[chunk * lon_n + pos] for pos in spots], axis=1)
            mixed = jnp.dot(mix_t[...], points, preferred_element_type=F32)
            for n, pos in enumerate(spots):
                row = row_at(chunk, pos)
                wet_row = mask_ref[pl.ds(row, 1), :].astype(F32)
                val = wet_row * (res[row].astype(F32) + mixed[:, n * cols : (n + 1) * cols])
                for h in range(tiles):
                    flat_out[h, pl.ds(row, channels, stride=rows), :] = val[:, h * LANES : (h + 1) * LANES]

    needs = [
        any((chunk * lon_n + q + HALO) % rows < HALO or (chunk * lon_n + q + HALO) % rows >= rows - HALO for q in range(lon_n))
        for chunk in range(per)]
    early = needs.index(True)
    if early:
        mix_rows(0, early)
    loads[7].wait()
    wide = modes // LANES
    for p in range(2):
        for t in range(wide):
            spec_ref[p, :, t * LANES : (t + 1) * LANES] = spec_raw[pl.ds(2 * t + p, channels, stride=2 * wide), :]
    loads[8].wait()
    if early > 1:
        pl.loop(0, early - 1)(spectral)
    await_halo()
    if early:
        spectral(early - 1)
    halo_conv()
    mix_rows(early, per)
    pl.loop(early, per)(spectral)
    if per > 1:
        pl.loop(0, per - 1)(finish)

    @pl.loop(0, per * (lon_n - 1))
    def _(at):
        chunk = at // (lon_n - 1)
        k = lon_n - 1 - lax.rem(at, lon_n - 1)
        send_row(chunk, k).wait_send()
        send_back(chunk, k).wait_send()

    finish(per - 1)

    @pl.loop(0, channels // step)
    def _(group):
        for u in range(step):
            c = group * step + u
            at = pl.multiple_of(c * rows, rows)
            for h in range(tiles):
                out_ref[c, :, h * LANES : (h + 1) * LANES] = flat_out[h, pl.ds(at, rows), :].astype(BF16)


def local(lat_n, lon_n, field, land_mask, fold_partner, dw_kernel, norm_gain, w_in, w_out, spec_gain, mix_weight):
    channels, rows, cols = field.shape
    modes = spec_gain.shape[2]
    hid = w_in.shape[1]
    lon_points = cols * lon_n
    hid_up = -(-hid // 16) * 16
    chan_up = -(-channels // LANES) * LANES
    tiles = cols // LANES
    table = jnp.asarray(dft_table(lon_points, modes))
    taps = dw_kernel.transpose(1, 2, 0)
    wide = modes // LANES
    spec = spec_gain.transpose(1, 0, 2).reshape(channels, 2, wide, LANES).transpose(0, 2, 1, 3).reshape(-1, LANES)
    per = rows // lon_n
    sizes = (channels, rows, cols, lat_n, lon_n, modes)
    operands = (field, land_mask, fold_partner[None, :], taps, norm_gain[None, :], w_in, w_out.T, mix_weight, spec, table)
    dma = pltpu.SemaphoreType.DMA
    peers = lon_n - 1
    return pl.pallas_call(
        functools.partial(kernel, sizes),
        out_shape=pltpu.VMEM(field.shape, BF16),
        in_specs=[pl.BlockSpec(memory_space=pltpu.HBM)] * len(operands),
        out_specs=pl.BlockSpec(memory_space=pltpu.VMEM),
        scratch_shapes=[
            *[pltpu.VMEM(x.shape, x.dtype) for x in operands],
            pltpu.VMEM((tiles, channels * rows, LANES), F32),
            pltpu.VMEM((rows, channels, cols), BF16),
            pltpu.VMEM((tiles, channels * rows, LANES), F32),
            pltpu.VMEM((tiles, channels * rows, LANES), F32),
            pltpu.VMEM((tiles + 1, channels * rows // 2, LANES), F32),
            pltpu.VMEM((channels, 4 * rows, LANES), BF16),
            pltpu.VMEM((LANES, chan_up), F32),
            *[pltpu.VMEM((channels, LANES), F32)] * 4,
            pltpu.VMEM((rows, channels, cols), BF16),
            pltpu.VMEM((per, channels, lon_points), BF16),
            pltpu.VMEM((per, channels, lon_points), BF16),
            pltpu.VMEM((rows, channels, cols), BF16),
            *[pltpu.VMEM((channels, LANES), BF16)] * 6,
            *[pltpu.VMEM((HALO, channels, cols), BF16)] * 2,
            pltpu.VMEM((HALO, channels, lon_points), BF16),
            pltpu.VMEM(spec_gain.shape, F32),
            pltpu.VMEM((hid_up, channels), BF16),
            pltpu.VMEM((channels, hid_up), BF16),
            pltpu.VMEM((channels, channels), BF16),
            pltpu.VMEM((channels, LANES), F32),
            dma((2 * len(operands) + channels,)),
            *[dma((2,))] * 6,
            *[dma((peers,))] * 2,
            *[dma((peers * per,))] * 4,
        ],
        compiler_params=pltpu.CompilerParams(
            collective_id=0, has_side_effects=True, vmem_limit_bytes=VMEM_LIMIT),
        name="block",
    )(*operands)


def solution(mesh):
    placed = (P(None, "lat", "lon"), P("lat", "lon"), P(), P(), P(), P(), P(), P(), P())
    return jax.shard_map(
        functools.partial(local, mesh.shape["lat"], mesh.shape["lon"]),
        mesh=mesh, in_specs=placed, out_specs=P(None, "lat", "lon"), check_vma=False,
    )
```

```python
import functools
import math

import jax
import jax.numpy as jnp
import numpy as np
from jax import lax
from jax.experimental import pallas as pl
from jax.experimental.pallas import tpu as pltpu
from jax.sharding import PartitionSpec as P

F32 = jnp.float32
BF16 = jnp.bfloat16
TAPS = 7
HALO = 3
LANES = 128
WORK = BF16
GELU_LINE = math.sqrt(2.0 / math.pi)
GELU_CUBE = 0.044715 * GELU_LINE
STEP = 30
VMEM_LIMIT = 58 * 1024 * 1024


def dft_table(lon_points, mode_count):
    phase = np.arange(lon_points)[:, None] * np.arange(mode_count)[None, :] % lon_points
    angles = phase.astype(np.float32) * np.float32(2.0 * math.pi / lon_points)
    factor = np.float32(1.0 / math.sqrt(lon_points))
    angles = angles.astype(np.float64)
    table = np.concatenate([np.cos(angles), -np.sin(angles)], axis=1).astype(np.float32)
    return (table * factor).astype(BF16)


def loop_step(channels):
    return max(u for u in range(2, STEP + 1, 2) if channels % u == 0)


def kernel(
    sizes,
    field_hbm, mask_hbm, fold_hbm, taps_hbm, gain_hbm, w_in_hbm, w_out_hbm, mix_hbm, spec_hbm, table_hbm,
    out_ref,
    field_ref, mask_ref, fold_ref, taps_ref, gain_ref, w_in_ref, w_out_ref, mix_ref, spec_raw, table_ref,
    flat, own, depth, flat_out, halo, toep, pattern_t, pattern, pattern_back, edge32, comb32,
    res, by_rows, back, spatial,
    edge_mine, edge_left, edge_right, comb, comb_n, comb_s, rows_n, rows_s, top_all,
    spec_ref, w_in_t, w_out_t, mix_t, gain_col,
    local_sem, edge_send, edge_recv, comb_send, comb_recv, rows_send, rows_recv,
    fold_send, fold_recv, out_send, out_recv, in_send, in_recv,
):
    channels, rows, cols, lat_n, lon_n, modes = sizes
    lon_points = cols * lon_n
    tiles = cols // LANES
    per = rows // lon_n
    step = loop_step(channels)
    lat = lax.axis_index("lat")
    lon = lax.axis_index("lon")
    left = lax.rem(lon + lon_n - 1, lon_n)
    right = lax.rem(lon + 1, lon_n)
    chip = lon // 2
    core = lax.rem(lon, 2)
    chips = lon_n // 2
    mate_core = chip * 2 + 1 - core

    def target(k):
        return lax.rem(chip + k // 2, chips) * 2 + lax.rem(core + lax.rem(k, 2), 2)

    def source(k):
        return lax.rem(chip + chips - k // 2, chips) * 2 + lax.rem(core + lax.rem(k, 2), 2)

    whole = (
        (taps_hbm, taps_ref), (mask_hbm, mask_ref), (fold_hbm, fold_ref), (gain_hbm, gain_ref), (w_in_hbm, w_in_ref),
        (w_out_hbm, w_out_ref), (mix_hbm, mix_ref), (spec_hbm, spec_raw), (table_hbm, table_ref))
    loads = [pltpu.make_async_copy(a, b, local_sem.at[n]) for n, (a, b) in enumerate(whole)]
    groups = channels // step

    def field_load(group):
        some = pl.ds(group * step, step)
        return pltpu.make_async_copy(field_hbm.at[some], field_ref.at[some], local_sem.at[len(whole) + group])

    loads[0].start()
    loads[1].start()
    for group in range(groups):
        field_load(group).start()

    barrier = pltpu.get_barrier_semaphore()
    for k in range(1, lon_n):
        pl.semaphore_signal(barrier, inc=1, device_id={"lon": target(k)})

    @pl.when(lat > 0)
    def _():
        pl.semaphore_signal(barrier, inc=1, device_id={"lat": lat - 1})

    @pl.when(lat < lat_n - 1)
    def _():
        pl.semaphore_signal(barrier, inc=1, device_id={"lat": lat + 1})

    lane = lax.broadcasted_iota(jnp.int32, (rows, LANES), 1)
    half = rows // 2
    loads[1].wait()
    wet = mask_ref[...].astype(F32)

    @pl.loop(0, channels // step)
    def _(group):
        for u in range(step):
            c = group * step + u
            if u == 0:
                field_load(group).wait()
            val = field_ref[c].astype(F32) * wet
            at = pl.multiple_of(c * rows, rows)
            parts = [val[:, h * LANES : (h + 1) * LANES] for h in range(tiles)]
            for h in range(tiles):
                flat[h, pl.ds(at, rows), :] = parts[h]
            edge = jnp.where(lane < HALO, parts[0], jnp.where(lane >= LANES - HALO, parts[-1], 0.0))
            edge = edge[:half] + pltpu.roll(edge[half:], LANES - 8 * half, 1)
            for hop in (4, 2, 1):
                edge = edge + pltpu.roll(pltpu.roll(edge, half - hop, 0), LANES - 8 * hop, 1)
            edge32[pl.ds(c, 1), :] = edge[:1]

    for load in loads[2:]:
        load.start()

    edge_mine[...] = edge32[...].astype(BF16)

    count = lon_n - 1 + jnp.where(lat > 0, 1, 0) + jnp.where(lat < lat_n - 1, 1, 0)
    pl.semaphore_wait(barrier, count)

    to_left = pltpu.make_async_remote_copy(
        edge_mine, edge_right, edge_send.at[0], edge_recv.at[0], device_id={"lon": left})
    to_right = pltpu.make_async_remote_copy(
        edge_mine, edge_left, edge_send.at[1], edge_recv.at[1], device_id={"lon": right})
    to_left.start()
    to_right.start()

    def own_row(i):
        for h in range(tiles):
            own[i, :, h * LANES : (h + 1) * LANES] = flat[h, pl.ds(i, channels, stride=rows), :].astype(BF16)

    rows_down = pltpu.make_async_remote_copy(
        own.at[pl.ds(0, HALO)], rows_n, rows_send.at[0], rows_recv.at[0], device_id={"lat": lat - 1})
    rows_up = pltpu.make_async_remote_copy(
        own.at[pl.ds(rows - HALO, HALO)], rows_s, rows_send.at[1], rows_recv.at[1], device_id={"lat": lat + 1})
    comb_down = pltpu.make_async_remote_copy(
        comb, comb_n, comb_send.at[0], comb_recv.at[0], device_id={"lat": lat - 1})
    comb_up = pltpu.make_async_remote_copy(
        comb, comb_s, comb_send.at[1], comb_recv.at[1], device_id={"lat": lat + 1})

    def piece(pos):
        return top_all.at[:, :, pl.ds(pl.multiple_of(pos * cols, LANES), cols)]

    def fold_out(j):
        whom = mate_core if j == 0 else lax.rem(chip + j, chips) * 2 + core
        return pltpu.make_async_remote_copy(
            own.at[pl.ds(rows - HALO, HALO)], piece(lon), fold_send.at[j], fold_recv.at[j], device_id={"lon": whom})

    def fold_pass(j):
        pos = lax.rem(chip + chips - j, chips) * 2 + core
        return pltpu.make_async_remote_copy(
            piece(pos), piece(pos), fold_send.at[chips + j - 1], fold_recv.at[chips + j - 1], device_id={"lon": mate_core})

    for i in range(rows - HALO, rows):
        own_row(i)

    @pl.when(lat < lat_n - 1)
    def _():
        rows_up.start()

    @pl.when(lat == lat_n - 1)
    def _():
        for j in range(chips - 1, -1, -1):
            fold_out(j).start()
        top_all[:, :, pl.ds(pl.multiple_of(lon * cols, LANES), cols)] = own[rows - HALO :]

    for i in range(HALO):
        own_row(i)

    @pl.when(lat > 0)
    def _():
        rows_down.start()

    loads[0].wait()
    pattern_t[...] = jnp.zeros(pattern_t.shape, F32)
    for a in range(TAPS):
        for b in range(TAPS):
            pattern_t[b * rows + a : b * rows + a + 1, :channels] = taps_ref[a, b : b + 1, :]
    pattern[...] = pattern_t[...].T[:channels]
    pattern_back[...] = pltpu.roll(pattern[...], LANES - HALO, 1)

    slot = lax.rem(lane, rows)
    index = lax.broadcasted_iota(jnp.int32, (rows, LANES), 0)
    band = jnp.abs(slot - index) <= HALO
    low_slot = slot[:half] < HALO
    high_slot = (slot[:half] >= half + HALO) & (slot[:half] < half + 2 * HALO)

    @pl.loop(0, channels // step)
    def _(group):
        for u in range(step):
            c = group * step + u
            row = jnp.broadcast_to(pattern_back[pl.ds(c, 1), :], (rows, LANES))
            mid = jnp.where(band, pltpu.roll(row, 0, 1, stride=1, stride_axis=0), 0.0)
            row = jnp.broadcast_to(pattern[pl.ds(c, 1), :], (half, LANES))
            far = pltpu.roll(row, 0, 1, stride=1, stride_axis=0)
            far = jnp.concatenate([jnp.where(low_slot, far, 0.0), jnp.where(high_slot, far, 0.0)], axis=0)
            for n, part in enumerate((mid, far)):
                coarse = part.astype(BF16)
                toep[c, 2 * n * rows : (2 * n + 1) * rows, :] = coarse
                toep[c, (2 * n + 1) * rows : (2 * n + 2) * rows, :] = (part - coarse.astype(F32)).astype(BF16)

    halo[...] = jnp.zeros(halo.shape, F32)

    def turned(ref, target_ref):
        n, m = ref.shape
        up = [-(-d // LANES) * LANES for d in (n, m)]
        full = jnp.concatenate([ref[...].astype(F32), jnp.zeros((n, up[1] - m), F32)], axis=1)
        full = jnp.concatenate([full, jnp.zeros((up[0] - n, up[1]), F32)], axis=0)
        target_ref[...] = full.T[: target_ref.shape[0], : target_ref.shape[1]].astype(BF16)

    for n in range(3, 7):
        loads[n].wait()
    turned(w_in_ref, w_in_t)
    w_out_t[...] = jnp.zeros(w_out_t.shape, BF16)
    w_out_t[:, : w_out_ref.shape[1]] = w_out_ref[...]
    turned(mix_ref, mix_t)
    diagonal = lax.broadcasted_iota(jnp.int32, (channels, channels), 0) == lax.broadcasted_iota(
        jnp.int32, (channels, channels), 1)
    gain_col[...] = jnp.broadcast_to(
        jnp.sum(jnp.where(diagonal, gain_ref[...], 0.0), axis=1, keepdims=True), (channels, LANES))

    for i in range(HALO, rows - HALO):
        own_row(i)

    to_left.wait()
    to_right.wait()
    near = lax.rem(lax.broadcasted_iota(jnp.int32, (channels, LANES), 1), 8) < 4
    both = jnp.where(near, edge_right[...].astype(F32), edge_left[...].astype(F32))
    comb[...] = both.astype(BF16)
    comb32[...] = both

    @pl.when(lat > 0)
    def _():
        comb_down.start()

    @pl.when(lat < lat_n - 1)
    def _():
        comb_up.start()

    def shifted(ring, finish_block):
        high = ring[0].shape[0]
        at = lane[:high]
        blocks = []
        for b in range(TAPS):
            d = b - HALO
            line = []
            for h in range(tiles):
                if d == 0:
                    line.append(ring[h])
                elif d > 0:
                    line.append(pltpu.roll(jnp.where(at < d, ring[h + 1], ring[h]), LANES - d, 1))
                else:
                    line.append(pltpu.roll(jnp.where(at >= LANES + d, ring[h - 1], ring[h]), -d, 1))
            blocks.append(finish_block(jnp.concatenate(line, axis=1)))
        return jnp.concatenate(blocks + [blocks[-1]] * (LANES // rows - TAPS), axis=0)

    blank = jnp.zeros((2 * rows, LANES), BF16)

    def product(c, which, rings, finish_block):
        span = slice(2 * which * rows, 2 * (which + 1) * rows)
        weights = jnp.concatenate(
            [jnp.concatenate([toep[c, span, :], blank], axis=1), jnp.concatenate([blank, toep[c + 1, span, :]], axis=1)],
            axis=0)
        points = jnp.concatenate([shifted(ring, finish_block) for ring in rings], axis=0)
        total = jnp.dot(weights, points, preferred_element_type=F32)
        return total[:rows] + total[rows : 2 * rows], total[2 * rows : 3 * rows] + total[3 * rows :]

    @pl.loop(0, channels // step)
    def _(group):
        for u in range(0, step, 2):
            rings = []
            for c in (group * step + u, group * step + u + 1):
                rim = jnp.broadcast_to(comb32[pl.ds(c, 1), :], (rows, LANES))
                rim = pltpu.roll(rim, 0, 1, stride=8, stride_axis=0)
                at = pl.multiple_of(c * rows, rows)
                rings.append([flat[h, pl.ds(at, rows), :].astype(WORK) for h in range(tiles)] + [rim.astype(WORK)])
            totals = product(group * step + u, 0, rings, lambda block: block.astype(BF16))
            for n, total in enumerate(totals):
                at = pl.multiple_of((group * step + u + n) * rows, rows)
                for h in range(tiles):
                    depth[h, pl.ds(at, rows), :] = total[:, h * LANES : (h + 1) * LANES]

    def edges_of(packed, i):
        return pltpu.roll(packed, 8 * i, 1) if i else packed

    def put_halo(at, value, rim):
        for h in range(tiles):
            halo[h, pl.ds(at, channels, stride=half), :] = value[:, h * LANES : (h + 1) * LANES]
        halo[tiles, pl.ds(at, channels, stride=half), :] = rim

    def await_halo():
        loads[2].wait()

        @pl.when(lat > 0)
        def _():
            rows_down.wait_send()
            comb_down.wait_send()
            rows_up.wait_recv()
            comb_up.wait_recv()
            for r in range(HALO):
                put_halo(r, rows_s[r].astype(F32), edges_of(comb_s[...].astype(F32), rows - HALO + r))

        @pl.when(lat < lat_n - 1)
        def _():
            rows_up.wait_send()
            comb_up.wait_send()
            rows_down.wait_recv()
            comb_down.wait_recv()
            for r in range(HALO):
                put_halo(HALO + r, rows_n[r].astype(F32), edges_of(comb_n[...].astype(F32), r))

        @pl.when(lat == lat_n - 1)
        def _():
            for j in range(1, chips):
                fold_out(j).wait_recv()
                fold_pass(j).start()
            for j in range(chips):
                fold_out(j).wait_send()
            fold_out(0).wait_recv()
            for j in range(1, chips):
                fold_pass(j).wait()
            point = lax.broadcasted_iota(jnp.int32, (lon_points, cols + LANES), 0)
            at = lax.broadcasted_iota(jnp.int32, (1, cols + LANES), 1)
            at = jnp.where(at < cols + HALO, at, at - (cols + LANES)) + lon * cols
            mate = fold_ref[:, :1] - at
            mate = jnp.where(mate < 0, mate + lon_points, mate)
            mate = jnp.where(mate < 0, mate + lon_points, mate)
            mate = jnp.where(mate >= lon_points, mate - lon_points, mate)
            pick = jnp.where(point == mate, 1.0, 0.0).astype(BF16)
            for r in range(HALO):
                row = jnp.dot(top_all[HALO - 1 - r], pick, preferred_element_type=F32)
                put_halo(HALO + r, row[:, :cols], row[:, cols:])

    def halo_conv():
        @pl.loop(0, channels // step)
        def _(group):
            for u in range(0, step, 2):
                rings = []
                for c in (group * step + u, group * step + u + 1):
                    spot = pl.ds(pl.multiple_of(c * half, half), half)
                    rings.append([halo[h, spot, :] for h in range(tiles + 1)])
                totals = product(
                    group * step + u, 1, rings, lambda block: jnp.concatenate([block, block], axis=0).astype(BF16))
                for n, total in enumerate(totals):
                    at = pl.multiple_of((group * step + u + n) * rows, rows)
                    for h in range(tiles):
                        depth[h, pl.ds(at, rows), :] += total[:, h * LANES : (h + 1) * LANES]

    here = pl.ds(pl.multiple_of(lon * cols, LANES), cols)

    def row_at(chunk, q):
        return lax.rem(chunk * lon_n + q + HALO, rows)

    def send_row(chunk, k):
        s = chunk * (lon_n - 1) + lon_n - 1 - k
        return pltpu.make_async_remote_copy(
            res.at[row_at(chunk, target(k))], by_rows.at[chunk, :, here],
            out_send.at[s], out_recv.at[s], device_id={"lon": target(k)})

    def send_back(chunk, k):
        q = target(k)
        s = chunk * (lon_n - 1) + lon_n - 1 - k
        return pltpu.make_async_remote_copy(
            back.at[chunk, :, pl.ds(pl.multiple_of(q * cols, LANES), cols)], spatial.at[chunk * lon_n + lon],
            in_send.at[s], in_recv.at[s], device_id={"lon": q})

    def mix_some(chunk, ks):
        places = [row_at(chunk, target(k)) for k in ks]
        x = jnp.concatenate(
            [depth[h, pl.ds(row, channels, stride=rows), :] for row in places for h in range(tiles)], axis=1)
        mean = jnp.sum(x, axis=0, keepdims=True) * (1.0 / channels)
        centred = x - mean
        var = jnp.sum(centred * centred, axis=0, keepdims=True) * (1.0 / channels)
        gain = jnp.concatenate([gain_col[...]] * (len(ks) * tiles), axis=1)
        normed = (centred * lax.rsqrt(var + 1e-06) * gain).astype(BF16)
        pre = jnp.dot(w_in_t[...], normed, preferred_element_type=F32)
        inner = pre * (GELU_CUBE * (pre * pre) + GELU_LINE)
        hidden = (pre + pre * jnp.tanh(inner)).astype(BF16)
        branch = jnp.dot(w_out_t[...], hidden, preferred_element_type=F32)
        for n, row in enumerate(places):
            wet_row = mask_ref[pl.ds(row, 1), :].astype(F32)
            part = 0.5 * branch[:, n * cols : (n + 1) * cols]
            res[row] = (wet_row * (own[row].astype(F32) + part)).astype(BF16)
        return places

    half_ring = lon_n // 2

    def mix_rows(first, last):
        @pl.loop(first, last)
        def _(at):
            chunk = at // half_ring
            pair = lax.rem(at, half_ring)
            k = lon_n - 1 - 2 * pair
            _, two = mix_some(chunk, (k, k - 1))
            send_row(chunk, k).start()

            @pl.when(pair < half_ring - 1)
            def _():
                send_row(chunk, k - 1).start()

            @pl.when(pair == half_ring - 1)
            def _():
                by_rows[chunk, :, here] = res[two]

    def mix_first():
        @pl.loop(0, 2)
        def _(at):
            mix_some(0, (lon_n - 1 - at,))
            send_row(0, lon_n - 1 - at).start()

    def spectral(chunk):
        for k in range(lon_n - 1, 0, -1):
            send_row(chunk, k).wait_recv()
        spectrum = jnp.dot(by_rows[chunk], table_ref[...], preferred_element_type=F32)
        s_re = spectrum[:, :modes]
        s_im = spectrum[:, modes:]
        g_re = spec_ref[0]
        g_im = spec_ref[1]
        scaled = jnp.concatenate(
            [(g_re * s_re - g_im * s_im).astype(BF16), (g_re * s_im + g_im * s_re).astype(BF16)], axis=1)
        back[chunk] = lax.dot_general(
            scaled, table_ref[...], (((1,), (1,)), ((), ())), preferred_element_type=F32).astype(BF16)
        for k in range(lon_n - 1, 0, -1):
            send_back(chunk, k).start()
        spatial[chunk * lon_n + lon] = back[chunk, :, here]

    def finish(chunk):
        @pl.loop(0, lon_n // 2)
        def _(pair):
            k = 2 * pair

            @pl.when(pair > 0)
            def _():
                send_back(chunk, k).wait_recv()

            send_back(chunk, k + 1).wait_recv()
            spots = [source(k), source(k + 1)]
            points = jnp.concatenate([spatial[chunk * lon_n + pos] for pos in spots], axis=1)
            mixed = jnp.dot(mix_t[...], points, preferred_element_type=F32)
            for n, pos in enumerate(spots):
                row = row_at(chunk, pos)
                wet_row = mask_ref[pl.ds(row, 1), :].astype(F32)
                val = wet_row * (res[row].astype(F32) + mixed[:, n * cols : (n + 1) * cols])
                for h in range(tiles):
                    flat_out[h, pl.ds(row, channels, stride=rows), :] = val[:, h * LANES : (h + 1) * LANES]

    needs = [
        any((chunk * lon_n + q + HALO) % rows < HALO or (chunk * lon_n + q + HALO) % rows >= rows - HALO for q in range(lon_n))
        for chunk in range(per)]
    early = needs.index(True)
    if early:
        alone = int(half_ring > 1)
        if alone:
            mix_first()
        mix_rows(alone, early * half_ring)
    loads[7].wait()
    wide = modes // LANES
    for p in range(2):
        for t in range(wide):
            spec_ref[p, :, t * LANES : (t + 1) * LANES] = spec_raw[pl.ds(2 * t + p, channels, stride=2 * wide), :]
    loads[8].wait()
    if early > 1:
        pl.loop(0, early - 1)(spectral)
    await_halo()
    if early:
        spectral(early - 1)
    halo_conv()
    mix_rows(early * half_ring, per * half_ring)
    pl.loop(early, per)(spectral)
    if per > 1:
        pl.loop(0, per - 1)(finish)

    @pl.loop(0, per * (lon_n - 1))
    def _(at):
        chunk = at // (lon_n - 1)
        k = lon_n - 1 - lax.rem(at, lon_n - 1)
        send_row(chunk, k).wait_send()
        send_back(chunk, k).wait_send()

    finish(per - 1)

    @pl.loop(0, channels // step)
    def _(group):
        for u in range(step):
            c = group * step + u
            at = pl.multiple_of(c * rows, rows)
            for h in range(tiles):
                out_ref[c, :, h * LANES : (h + 1) * LANES] = flat_out[h, pl.ds(at, rows), :].astype(BF16)


def local(lat_n, lon_n, field, land_mask, fold_partner, dw_kernel, norm_gain, w_in, w_out, spec_gain, mix_weight):
    channels, rows, cols = field.shape
    modes = spec_gain.shape[2]
    hid = w_in.shape[1]
    lon_points = cols * lon_n
    hid_up = -(-hid // 16) * 16
    chan_up = -(-channels // LANES) * LANES
    tiles = cols // LANES
    table = jnp.asarray(dft_table(lon_points, modes))
    taps = dw_kernel.transpose(1, 2, 0)
    wide = modes // LANES
    spec = spec_gain.transpose(1, 0, 2).reshape(channels, 2, wide, LANES).transpose(0, 2, 1, 3).reshape(-1, LANES)
    per = rows // lon_n
    groups = channels // loop_step(channels)
    sizes = (channels, rows, cols, lat_n, lon_n, modes)
    operands = (field, land_mask, fold_partner[None, :], taps, norm_gain[None, :], w_in, w_out.T, mix_weight, spec, table)
    dma = pltpu.SemaphoreType.DMA
    peers = lon_n - 1
    return pl.pallas_call(
        functools.partial(kernel, sizes),
        out_shape=pltpu.VMEM(field.shape, BF16),
        in_specs=[pl.BlockSpec(memory_space=pltpu.HBM)] * len(operands),
        out_specs=pl.BlockSpec(memory_space=pltpu.VMEM),
        scratch_shapes=[
            *[pltpu.VMEM(x.shape, x.dtype) for x in operands],
            pltpu.VMEM((tiles, channels * rows, LANES), F32),
            pltpu.VMEM((rows, channels, cols), BF16),
            pltpu.VMEM((tiles, channels * rows, LANES), F32),
            pltpu.VMEM((tiles, channels * rows, LANES), F32),
            pltpu.VMEM((tiles + 1, channels * rows // 2, LANES), F32),
            pltpu.VMEM((channels, 4 * rows, LANES), BF16),
            pltpu.VMEM((LANES, chan_up), F32),
            *[pltpu.VMEM((channels, LANES), F32)] * 4,
            pltpu.VMEM((rows, channels, cols), BF16),
            pltpu.VMEM((per, channels, lon_points), BF16),
            pltpu.VMEM((per, channels, lon_points), BF16),
            pltpu.VMEM((rows, channels, cols), BF16),
            *[pltpu.VMEM((channels, LANES), BF16)] * 6,
            *[pltpu.VMEM((HALO, channels, cols), BF16)] * 2,
            pltpu.VMEM((HALO, channels, lon_points), BF16),
            pltpu.VMEM(spec_gain.shape, F32),
            pltpu.VMEM((hid_up, channels), BF16),
            pltpu.VMEM((channels, hid_up), BF16),
            pltpu.VMEM((channels, channels), BF16),
            pltpu.VMEM((channels, LANES), F32),
            dma((len(operands) + groups,)),
            *[dma((2,))] * 6,
            *[dma((peers,))] * 2,
            *[dma((peers * per,))] * 4,
        ],
        compiler_params=pltpu.CompilerParams(
            collective_id=0, has_side_effects=True, vmem_limit_bytes=VMEM_LIMIT),
        name="block",
    )(*operands)


def solution(mesh):
    placed = (P(None, "lat", "lon"), P("lat", "lon"), P(), P(), P(), P(), P(), P(), P())
    return jax.shard_map(
        functools.partial(local, mesh.shape["lat"], mesh.shape["lon"]),
        mesh=mesh, in_specs=placed, out_specs=P(None, "lat", "lon"), check_vma=False,
    )
```

```python
import functools
import math

import jax
import jax.numpy as jnp
import numpy as np
from jax import lax
from jax.experimental import pallas as pl
from jax.experimental.pallas import tpu as pltpu
from jax.sharding import PartitionSpec as P

F32 = jnp.float32
BF16 = jnp.bfloat16
TAPS = 7
HALO = 3
LANES = 128
WORK = BF16
GELU_LINE = math.sqrt(2.0 / math.pi)
GELU_CUBE = 0.044715 * GELU_LINE
STEP = 30
VMEM_LIMIT = 58 * 1024 * 1024


def dft_table(lon_points, mode_count):
    phase = np.arange(lon_points)[:, None] * np.arange(mode_count)[None, :] % lon_points
    angles = phase.astype(np.float32) * np.float32(2.0 * math.pi / lon_points)
    factor = np.float32(1.0 / math.sqrt(lon_points))
    angles = angles.astype(np.float64)
    table = np.concatenate([np.cos(angles), -np.sin(angles)], axis=1).astype(np.float32)
    return (table * factor).astype(BF16)


def loop_step(channels):
    return max(u for u in range(2, STEP + 1, 2) if channels % u == 0)


def kernel(
    sizes,
    field_hbm, mask_hbm, fold_hbm, taps_hbm, gain_hbm, w_in_hbm, w_out_hbm, mix_hbm, spec_hbm, table_hbm,
    out_ref,
    field_ref, mask_ref, fold_ref, taps_ref, gain_ref, w_in_ref, w_out_ref, mix_ref, spec_raw, table_ref,
    flat, own, depth, flat_out, halo, toep, pattern_t, pattern, pattern_back, edge32, comb32,
    res, by_rows, back, spatial,
    edge_mine, edge_left, edge_right, comb, comb_n, comb_s, rows_n, rows_s, top_all,
    spec_ref, w_in_t, w_out_t, mix_t, gain_col,
    local_sem, edge_send, edge_recv, comb_send, comb_recv, rows_send, rows_recv,
    fold_send, fold_recv, out_send, out_recv, in_send, in_recv,
):
    channels, rows, cols, lat_n, lon_n, modes = sizes
    lon_points = cols * lon_n
    tiles = cols // LANES
    per = rows // lon_n
    step = loop_step(channels)
    lat = lax.axis_index("lat")
    lon = lax.axis_index("lon")
    left = lax.rem(lon + lon_n - 1, lon_n)
    right = lax.rem(lon + 1, lon_n)
    chip = lon // 2
    core = lax.rem(lon, 2)
    chips = lon_n // 2
    mate_core = chip * 2 + 1 - core

    def target(k):
        return lax.rem(chip + k // 2, chips) * 2 + lax.rem(core + lax.rem(k, 2), 2)

    def source(k):
        return lax.rem(chip + chips - k // 2, chips) * 2 + lax.rem(core + lax.rem(k, 2), 2)

    whole = (
        (taps_hbm, taps_ref), (mask_hbm, mask_ref), (fold_hbm, fold_ref), (gain_hbm, gain_ref), (w_in_hbm, w_in_ref),
        (w_out_hbm, w_out_ref), (mix_hbm, mix_ref), (spec_hbm, spec_raw), (table_hbm, table_ref))
    loads = [pltpu.make_async_copy(a, b, local_sem.at[n]) for n, (a, b) in enumerate(whole)]
    groups = channels // step

    def field_load(group):
        some = pl.ds(group * step, step)
        return pltpu.make_async_copy(field_hbm.at[some], field_ref.at[some], local_sem.at[len(whole) + group])

    loads[0].start()
    loads[1].start()
    for group in range(groups):
        field_load(group).start()

    barrier = pltpu.get_barrier_semaphore()
    for k in range(1, lon_n):
        pl.semaphore_signal(barrier, inc=1, device_id={"lon": target(k)})

    @pl.when(lat > 0)
    def _():
        pl.semaphore_signal(barrier, inc=1, device_id={"lat": lat - 1})

    @pl.when(lat < lat_n - 1)
    def _():
        pl.semaphore_signal(barrier, inc=1, device_id={"lat": lat + 1})

    lane = lax.broadcasted_iota(jnp.int32, (rows, LANES), 1)
    half = rows // 2
    loads[1].wait()
    wet = mask_ref[...].astype(F32)

    def mask_group(group):
        for u in range(step):
            c = group * step + u
            if u == 0:
                field_load(group).wait()
            val = field_ref[c].astype(F32) * wet
            at = pl.multiple_of(c * rows, rows)
            parts = [val[:, h * LANES : (h + 1) * LANES] for h in range(tiles)]
            for h in range(tiles):
                flat[h, pl.ds(at, rows), :] = parts[h]
            edge = jnp.where(lane < HALO, parts[0], jnp.where(lane >= LANES - HALO, parts[-1], 0.0))
            edge = edge[:half] + pltpu.roll(edge[half:], LANES - 8 * half, 1)
            for hop in (4, 2, 1):
                edge = edge + pltpu.roll(pltpu.roll(edge, half - hop, 0), LANES - 8 * hop, 1)
            edge32[pl.ds(c, 1), :] = edge[:1]

    first_groups = -(-groups // 2)
    split_at = first_groups * step // 16 * 16
    parts = (slice(0, split_at), slice(split_at, channels))

    def edge_copy(n, way):
        some = pl.ds(parts[n].start, parts[n].stop - parts[n].start)
        put = (edge_right, edge_left)[way]
        return pltpu.make_async_remote_copy(
            edge_mine.at[some], put.at[some], edge_send.at[2 * n + way], edge_recv.at[2 * n + way],
            device_id={"lon": (left, right)[way]})

    def send_edges(n):
        edge_mine[parts[n], :] = edge32[parts[n], :].astype(BF16)
        edge_copy(n, 0).start()
        edge_copy(n, 1).start()

    count = lon_n - 1 + jnp.where(lat > 0, 1, 0) + jnp.where(lat < lat_n - 1, 1, 0)
    pl.loop(0, first_groups)(mask_group)
    pl.semaphore_wait(barrier, count)
    send_edges(0)
    pl.loop(first_groups, groups)(mask_group)
    send_edges(1)
    for load in loads[2:]:
        load.start()

    def own_row(i):
        for h in range(tiles):
            own[i, :, h * LANES : (h + 1) * LANES] = flat[h, pl.ds(i, channels, stride=rows), :].astype(BF16)

    rows_down = pltpu.make_async_remote_copy(
        own.at[pl.ds(0, HALO)], rows_n, rows_send.at[0], rows_recv.at[0], device_id={"lat": lat - 1})
    rows_up = pltpu.make_async_remote_copy(
        own.at[pl.ds(rows - HALO, HALO)], rows_s, rows_send.at[1], rows_recv.at[1], device_id={"lat": lat + 1})
    comb_down = pltpu.make_async_remote_copy(
        comb, comb_n, comb_send.at[0], comb_recv.at[0], device_id={"lat": lat - 1})
    comb_up = pltpu.make_async_remote_copy(
        comb, comb_s, comb_send.at[1], comb_recv.at[1], device_id={"lat": lat + 1})

    def piece(pos):
        return top_all.at[:, :, pl.ds(pl.multiple_of(pos * cols, LANES), cols)]

    def fold_out(j):
        whom = mate_core if j == 0 else lax.rem(chip + j, chips) * 2 + core
        return pltpu.make_async_remote_copy(
            own.at[pl.ds(rows - HALO, HALO)], piece(lon), fold_send.at[j], fold_recv.at[j], device_id={"lon": whom})

    def fold_pass(j):
        pos = lax.rem(chip + chips - j, chips) * 2 + core
        return pltpu.make_async_remote_copy(
            piece(pos), piece(pos), fold_send.at[chips + j - 1], fold_recv.at[chips + j - 1], device_id={"lon": mate_core})

    for i in range(rows - HALO, rows):
        own_row(i)

    @pl.when(lat < lat_n - 1)
    def _():
        rows_up.start()

    @pl.when(lat == lat_n - 1)
    def _():
        for j in range(chips - 1, -1, -1):
            fold_out(j).start()
        top_all[:, :, pl.ds(pl.multiple_of(lon * cols, LANES), cols)] = own[rows - HALO :]

    for i in range(HALO):
        own_row(i)

    @pl.when(lat > 0)
    def _():
        rows_down.start()

    loads[0].wait()
    pattern_t[...] = jnp.zeros(pattern_t.shape, F32)
    for a in range(TAPS):
        for b in range(TAPS):
            pattern_t[b * rows + a : b * rows + a + 1, :channels] = taps_ref[a, b : b + 1, :]
    pattern[...] = pattern_t[...].T[:channels]
    pattern_back[...] = pltpu.roll(pattern[...], LANES - HALO, 1)

    slot = lax.rem(lane, rows)
    index = lax.broadcasted_iota(jnp.int32, (rows, LANES), 0)
    band = jnp.abs(slot - index) <= HALO
    low_slot = slot[:half] < HALO
    high_slot = (slot[:half] >= half + HALO) & (slot[:half] < half + 2 * HALO)

    @pl.loop(0, channels // step)
    def _(group):
        for u in range(step):
            c = group * step + u
            row = jnp.broadcast_to(pattern_back[pl.ds(c, 1), :], (rows, LANES))
            mid = jnp.where(band, pltpu.roll(row, 0, 1, stride=1, stride_axis=0), 0.0)
            row = jnp.broadcast_to(pattern[pl.ds(c, 1), :], (half, LANES))
            far = pltpu.roll(row, 0, 1, stride=1, stride_axis=0)
            far = jnp.concatenate([jnp.where(low_slot, far, 0.0), jnp.where(high_slot, far, 0.0)], axis=0)
            for n, part in enumerate((mid, far)):
                coarse = part.astype(BF16)
                toep[c, 2 * n * rows : (2 * n + 1) * rows, :] = coarse
                toep[c, (2 * n + 1) * rows : (2 * n + 2) * rows, :] = (part - coarse.astype(F32)).astype(BF16)

    halo[...] = jnp.zeros(halo.shape, F32)

    def turned(ref, target_ref):
        n, m = ref.shape
        up = [-(-d // LANES) * LANES for d in (n, m)]
        full = jnp.concatenate([ref[...].astype(F32), jnp.zeros((n, up[1] - m), F32)], axis=1)
        full = jnp.concatenate([full, jnp.zeros((up[0] - n, up[1]), F32)], axis=0)
        target_ref[...] = full.T[: target_ref.shape[0], : target_ref.shape[1]].astype(BF16)

    for n in range(3, 7):
        loads[n].wait()
    turned(w_in_ref, w_in_t)
    w_out_t[...] = jnp.zeros(w_out_t.shape, BF16)
    w_out_t[:, : w_out_ref.shape[1]] = w_out_ref[...]
    turned(mix_ref, mix_t)
    diagonal = lax.broadcasted_iota(jnp.int32, (channels, channels), 0) == lax.broadcasted_iota(
        jnp.int32, (channels, channels), 1)
    gain_col[...] = jnp.broadcast_to(
        jnp.sum(jnp.where(diagonal, gain_ref[...], 0.0), axis=1, keepdims=True), (channels, LANES))

    for i in range(HALO, rows - HALO):
        own_row(i)

    def take_edges(n):
        edge_copy(n, 0).wait()
        edge_copy(n, 1).wait()
        part = parts[n]
        near = lax.rem(lax.broadcasted_iota(jnp.int32, (part.stop - part.start, LANES), 1), 8) < 4
        both = jnp.where(near, edge_right[part, :].astype(F32), edge_left[part, :].astype(F32))
        comb[part, :] = both.astype(BF16)
        comb32[part, :] = both

    def shifted(ring, finish_block):
        high = ring[0].shape[0]
        at = lane[:high]
        blocks = []
        for b in range(TAPS):
            d = b - HALO
            line = []
            for h in range(tiles):
                if d == 0:
                    line.append(ring[h])
                elif d > 0:
                    line.append(pltpu.roll(jnp.where(at < d, ring[h + 1], ring[h]), LANES - d, 1))
                else:
                    line.append(pltpu.roll(jnp.where(at >= LANES + d, ring[h - 1], ring[h]), -d, 1))
            blocks.append(finish_block(jnp.concatenate(line, axis=1)))
        return jnp.concatenate(blocks + [blocks[-1]] * (LANES // rows - TAPS), axis=0)

    blank = jnp.zeros((2 * rows, LANES), BF16)

    def product(c, which, rings, finish_block):
        span = slice(2 * which * rows, 2 * (which + 1) * rows)
        weights = jnp.concatenate(
            [jnp.concatenate([toep[c, span, :], blank], axis=1), jnp.concatenate([blank, toep[c + 1, span, :]], axis=1)],
            axis=0)
        points = jnp.concatenate([shifted(ring, finish_block) for ring in rings], axis=0)
        total = jnp.dot(weights, points, preferred_element_type=F32)
        return total[:rows] + total[rows : 2 * rows], total[2 * rows : 3 * rows] + total[3 * rows :]

    def conv_group(group):
        for u in range(0, step, 2):
            rings = []
            for c in (group * step + u, group * step + u + 1):
                rim = jnp.broadcast_to(comb32[pl.ds(c, 1), :], (rows, LANES))
                rim = pltpu.roll(rim, 0, 1, stride=8, stride_axis=0)
                at = pl.multiple_of(c * rows, rows)
                rings.append([flat[h, pl.ds(at, rows), :].astype(WORK) for h in range(tiles)] + [rim.astype(WORK)])
            totals = product(group * step + u, 0, rings, lambda block: block.astype(BF16))
            for n, total in enumerate(totals):
                at = pl.multiple_of((group * step + u + n) * rows, rows)
                for h in range(tiles):
                    depth[h, pl.ds(at, rows), :] = total[:, h * LANES : (h + 1) * LANES]

    take_edges(0)
    pl.loop(0, split_at // step)(conv_group)
    take_edges(1)

    @pl.when(lat > 0)
    def _():
        comb_down.start()

    @pl.when(lat < lat_n - 1)
    def _():
        comb_up.start()

    pl.loop(split_at // step, groups)(conv_group)

    def edges_of(packed, i):
        return pltpu.roll(packed, 8 * i, 1) if i else packed

    def put_halo(at, value, rim):
        for h in range(tiles):
            halo[h, pl.ds(at, channels, stride=half), :] = value[:, h * LANES : (h + 1) * LANES]
        halo[tiles, pl.ds(at, channels, stride=half), :] = rim

    def await_halo():
        loads[2].wait()

        @pl.when(lat > 0)
        def _():
            rows_down.wait_send()
            comb_down.wait_send()
            rows_up.wait_recv()
            comb_up.wait_recv()
            for r in range(HALO):
                put_halo(r, rows_s[r].astype(F32), edges_of(comb_s[...].astype(F32), rows - HALO + r))

        @pl.when(lat < lat_n - 1)
        def _():
            rows_up.wait_send()
            comb_up.wait_send()
            rows_down.wait_recv()
            comb_down.wait_recv()
            for r in range(HALO):
                put_halo(HALO + r, rows_n[r].astype(F32), edges_of(comb_n[...].astype(F32), r))

        @pl.when(lat == lat_n - 1)
        def _():
            for j in range(1, chips):
                fold_out(j).wait_recv()
                fold_pass(j).start()
            for j in range(chips):
                fold_out(j).wait_send()
            fold_out(0).wait_recv()
            for j in range(1, chips):
                fold_pass(j).wait()
            point = lax.broadcasted_iota(jnp.int32, (lon_points, cols + LANES), 0)
            at = lax.broadcasted_iota(jnp.int32, (1, cols + LANES), 1)
            at = jnp.where(at < cols + HALO, at, at - (cols + LANES)) + lon * cols
            mate = fold_ref[:, :1] - at
            mate = jnp.where(mate < 0, mate + lon_points, mate)
            mate = jnp.where(mate < 0, mate + lon_points, mate)
            mate = jnp.where(mate >= lon_points, mate - lon_points, mate)
            pick = jnp.where(point == mate, 1.0, 0.0).astype(BF16)
            for r in range(HALO):
                row = jnp.dot(top_all[HALO - 1 - r], pick, preferred_element_type=F32)
                put_halo(HALO + r, row[:, :cols], row[:, cols:])

    def halo_conv():
        @pl.loop(0, channels // step)
        def _(group):
            for u in range(0, step, 2):
                rings = []
                for c in (group * step + u, group * step + u + 1):
                    spot = pl.ds(pl.multiple_of(c * half, half), half)
                    rings.append([halo[h, spot, :] for h in range(tiles + 1)])
                totals = product(
                    group * step + u, 1, rings, lambda block: jnp.concatenate([block, block], axis=0).astype(BF16))
                for n, total in enumerate(totals):
                    at = pl.multiple_of((group * step + u + n) * rows, rows)
                    for h in range(tiles):
                        depth[h, pl.ds(at, rows), :] += total[:, h * LANES : (h + 1) * LANES]

    here = pl.ds(pl.multiple_of(lon * cols, LANES), cols)

    def row_at(chunk, q):
        return lax.rem(chunk * lon_n + q + HALO, rows)

    def send_row(chunk, k):
        s = chunk * (lon_n - 1) + lon_n - 1 - k
        return pltpu.make_async_remote_copy(
            res.at[row_at(chunk, target(k))], by_rows.at[chunk, :, here],
            out_send.at[s], out_recv.at[s], device_id={"lon": target(k)})

    def send_back(chunk, k):
        q = target(k)
        s = chunk * (lon_n - 1) + lon_n - 1 - k
        return pltpu.make_async_remote_copy(
            back.at[chunk, :, pl.ds(pl.multiple_of(q * cols, LANES), cols)], spatial.at[chunk * lon_n + lon],
            in_send.at[s], in_recv.at[s], device_id={"lon": q})

    def mix_some(chunk, ks):
        places = [row_at(chunk, target(k)) for k in ks]
        x = jnp.concatenate(
            [depth[h, pl.ds(row, channels, stride=rows), :] for row in places for h in range(tiles)], axis=1)
        mean = jnp.sum(x, axis=0, keepdims=True) * (1.0 / channels)
        centred = x - mean
        var = jnp.sum(centred * centred, axis=0, keepdims=True) * (1.0 / channels)
        gain = jnp.concatenate([gain_col[...]] * (len(ks) * tiles), axis=1)
        normed = (centred * lax.rsqrt(var + 1e-06) * gain).astype(BF16)
        pre = jnp.dot(w_in_t[...], normed, preferred_element_type=F32)
        inner = pre * (GELU_CUBE * (pre * pre) + GELU_LINE)
        hidden = (pre + pre * jnp.tanh(inner)).astype(BF16)
        branch = jnp.dot(w_out_t[...], hidden, preferred_element_type=F32)
        for n, row in enumerate(places):
            wet_row = mask_ref[pl.ds(row, 1), :].astype(F32)
            part = 0.5 * branch[:, n * cols : (n + 1) * cols]
            res[row] = (wet_row * (own[row].astype(F32) + part)).astype(BF16)
        return places

    half_ring = lon_n // 2

    def mix_rows(first, last):
        @pl.loop(first, last)
        def _(at):
            chunk = at // half_ring
            pair = lax.rem(at, half_ring)
            k = lon_n - 1 - 2 * pair
            _, two = mix_some(chunk, (k, k - 1))
            send_row(chunk, k).start()

            @pl.when(pair < half_ring - 1)
            def _():
                send_row(chunk, k - 1).start()

            @pl.when(pair == half_ring - 1)
            def _():
                by_rows[chunk, :, here] = res[two]

    alone = int(half_ring > 1)

    def mix_first(chunk):
        @pl.loop(0, 2 * alone)
        def _(at):
            mix_some(chunk, (lon_n - 1 - at,))
            send_row(chunk, lon_n - 1 - at).start()

    def spectral(chunk):
        for k in range(lon_n - 1, 0, -1):
            send_row(chunk, k).wait_recv()
        spectrum = jnp.dot(by_rows[chunk], table_ref[...], preferred_element_type=F32)
        s_re = spectrum[:, :modes]
        s_im = spectrum[:, modes:]
        g_re = spec_ref[0]
        g_im = spec_ref[1]
        scaled = jnp.concatenate(
            [(g_re * s_re - g_im * s_im).astype(BF16), (g_re * s_im + g_im * s_re).astype(BF16)], axis=1)
        back[chunk] = lax.dot_general(
            scaled, table_ref[...], (((1,), (1,)), ((), ())), preferred_element_type=F32).astype(BF16)
        for k in range(lon_n - 1, 0, -1):
            send_back(chunk, k).start()
        spatial[chunk * lon_n + lon] = back[chunk, :, here]

    def finish(chunk):
        @pl.loop(0, lon_n // 2)
        def _(pair):
            k = 2 * pair

            @pl.when(pair > 0)
            def _():
                send_back(chunk, k).wait_recv()

            send_back(chunk, k + 1).wait_recv()
            spots = [source(k), source(k + 1)]
            points = jnp.concatenate([spatial[chunk * lon_n + pos] for pos in spots], axis=1)
            mixed = jnp.dot(mix_t[...], points, preferred_element_type=F32)
            for n, pos in enumerate(spots):
                row = row_at(chunk, pos)
                wet_row = mask_ref[pl.ds(row, 1), :].astype(F32)
                val = wet_row * (res[row].astype(F32) + mixed[:, n * cols : (n + 1) * cols])
                for h in range(tiles):
                    flat_out[h, pl.ds(row, channels, stride=rows), :] = val[:, h * LANES : (h + 1) * LANES]

    needs = [
        any((chunk * lon_n + q + HALO) % rows < HALO or (chunk * lon_n + q + HALO) % rows >= rows - HALO for q in range(lon_n))
        for chunk in range(per)]
    early = needs.index(True)
    if early:
        mix_first(0)
        mix_rows(alone, early * half_ring)
    loads[7].wait()
    wide = modes // LANES
    for p in range(2):
        for t in range(wide):
            spec_ref[p, :, t * LANES : (t + 1) * LANES] = spec_raw[pl.ds(2 * t + p, channels, stride=2 * wide), :]
    loads[8].wait()
    if early > 1:
        pl.loop(0, early - 1)(spectral)
    await_halo()
    if early:
        spectral(early - 1)
    halo_conv()
    mix_first(early)
    mix_rows(early * half_ring + alone, per * half_ring)
    pl.loop(early, per)(spectral)
    if per > 1:
        pl.loop(0, per - 1)(finish)

    @pl.loop(0, per * (lon_n - 1))
    def _(at):
        chunk = at // (lon_n - 1)
        k = lon_n - 1 - lax.rem(at, lon_n - 1)
        send_row(chunk, k).wait_send()
        send_back(chunk, k).wait_send()

    finish(per - 1)

    @pl.loop(0, channels // step)
    def _(group):
        for u in range(step):
            c = group * step + u
            at = pl.multiple_of(c * rows, rows)
            for h in range(tiles):
                out_ref[c, :, h * LANES : (h + 1) * LANES] = flat_out[h, pl.ds(at, rows), :].astype(BF16)


def local(lat_n, lon_n, field, land_mask, fold_partner, dw_kernel, norm_gain, w_in, w_out, spec_gain, mix_weight):
    channels, rows, cols = field.shape
    modes = spec_gain.shape[2]
    hid = w_in.shape[1]
    lon_points = cols * lon_n
    hid_up = -(-hid // 16) * 16
    chan_up = -(-channels // LANES) * LANES
    tiles = cols // LANES
    table = jnp.asarray(dft_table(lon_points, modes))
    taps = dw_kernel.transpose(1, 2, 0)
    wide = modes // LANES
    spec = spec_gain.transpose(1, 0, 2).reshape(channels, 2, wide, LANES).transpose(0, 2, 1, 3).reshape(-1, LANES)
    per = rows // lon_n
    groups = channels // loop_step(channels)
    sizes = (channels, rows, cols, lat_n, lon_n, modes)
    operands = (field, land_mask, fold_partner[None, :], taps, norm_gain[None, :], w_in, w_out.T, mix_weight, spec, table)
    dma = pltpu.SemaphoreType.DMA
    peers = lon_n - 1
    return pl.pallas_call(
        functools.partial(kernel, sizes),
        out_shape=pltpu.VMEM(field.shape, BF16),
        in_specs=[pl.BlockSpec(memory_space=pltpu.HBM)] * len(operands),
        out_specs=pl.BlockSpec(memory_space=pltpu.VMEM),
        scratch_shapes=[
            *[pltpu.VMEM(x.shape, x.dtype) for x in operands],
            pltpu.VMEM((tiles, channels * rows, LANES), F32),
            pltpu.VMEM((rows, channels, cols), BF16),
            pltpu.VMEM((tiles, channels * rows, LANES), F32),
            pltpu.VMEM((tiles, channels * rows, LANES), F32),
            pltpu.VMEM((tiles + 1, channels * rows // 2, LANES), F32),
            pltpu.VMEM((channels, 4 * rows, LANES), BF16),
            pltpu.VMEM((LANES, chan_up), F32),
            *[pltpu.VMEM((channels, LANES), F32)] * 4,
            pltpu.VMEM((rows, channels, cols), BF16),
            pltpu.VMEM((per, channels, lon_points), BF16),
            pltpu.VMEM((per, channels, lon_points), BF16),
            pltpu.VMEM((rows, channels, cols), BF16),
            *[pltpu.VMEM((channels, LANES), BF16)] * 6,
            *[pltpu.VMEM((HALO, channels, cols), BF16)] * 2,
            pltpu.VMEM((HALO, channels, lon_points), BF16),
            pltpu.VMEM(spec_gain.shape, F32),
            pltpu.VMEM((hid_up, channels), BF16),
            pltpu.VMEM((channels, hid_up), BF16),
            pltpu.VMEM((channels, channels), BF16),
            pltpu.VMEM((channels, LANES), F32),
            dma((len(operands) + groups,)),
            *[dma((4,))] * 2,
            *[dma((2,))] * 4,
            *[dma((peers,))] * 2,
            *[dma((peers * per,))] * 4,
        ],
        compiler_params=pltpu.CompilerParams(
            collective_id=0, has_side_effects=True, vmem_limit_bytes=VMEM_LIMIT),
        name="block",
    )(*operands)


def solution(mesh):
    placed = (P(None, "lat", "lon"), P("lat", "lon"), P(), P(), P(), P(), P(), P(), P())
    return jax.shard_map(
        functools.partial(local, mesh.shape["lat"], mesh.shape["lon"]),
        mesh=mesh, in_specs=placed, out_specs=P(None, "lat", "lon"), check_vma=False,
    )
```

```python
import functools
import math

import jax
import jax.numpy as jnp
import numpy as np
from jax import lax
from jax.experimental import pallas as pl
from jax.experimental.pallas import tpu as pltpu
from jax.sharding import PartitionSpec as P

F32 = jnp.float32
BF16 = jnp.bfloat16
TAPS = 7
HALO = 3
LANES = 128
WORK = BF16
GELU_LINE = math.sqrt(2.0 / math.pi)
GELU_CUBE = 0.044715 * GELU_LINE
STEP = 30
VMEM_LIMIT = 58 * 1024 * 1024


def dft_table(lon_points, mode_count):
    phase = np.arange(lon_points)[:, None] * np.arange(mode_count)[None, :] % lon_points
    angles = phase.astype(np.float32) * np.float32(2.0 * math.pi / lon_points)
    factor = np.float32(1.0 / math.sqrt(lon_points))
    angles = angles.astype(np.float64)
    table = np.concatenate([np.cos(angles), -np.sin(angles)], axis=1).astype(np.float32)
    return (table * factor).astype(BF16)


def loop_step(channels):
    return max(u for u in range(2, STEP + 1, 2) if channels % u == 0)


def kernel(
    sizes,
    field_hbm, mask_hbm, fold_hbm, taps_hbm, gain_hbm, w_in_hbm, w_out_hbm, mix_hbm, spec_hbm, table_hbm,
    out_ref,
    field_ref, mask_ref, fold_ref, taps_ref, gain_ref, w_in_ref, w_out_ref, mix_ref, spec_raw, table_ref,
    flat, own, depth, flat_out, halo, toep, pattern_t, pattern, pattern_back, edge32, comb32,
    res, by_rows, back, spatial,
    edge_mine, edge_left, edge_right, comb, comb_n, comb_s, rows_n, rows_s, top_all,
    spec_ref, w_in_t, w_out_t, mix_t, gain_col,
    local_sem, edge_send, edge_recv, comb_send, comb_recv, rows_send, rows_recv,
    fold_send, fold_recv, out_send, out_recv, in_send, in_recv,
):
    channels, rows, cols, lat_n, lon_n, modes = sizes
    lon_points = cols * lon_n
    tiles = cols // LANES
    per = rows // lon_n
    step = loop_step(channels)
    lat = lax.axis_index("lat")
    lon = lax.axis_index("lon")
    left = lax.rem(lon + lon_n - 1, lon_n)
    right = lax.rem(lon + 1, lon_n)
    chip = lon // 2
    core = lax.rem(lon, 2)
    chips = lon_n // 2
    mate_core = chip * 2 + 1 - core

    def target(k):
        return lax.rem(chip + k // 2, chips) * 2 + lax.rem(core + lax.rem(k, 2), 2)

    def source(k):
        return lax.rem(chip + chips - k // 2, chips) * 2 + lax.rem(core + lax.rem(k, 2), 2)

    whole = (
        (taps_hbm, taps_ref), (mask_hbm, mask_ref), (fold_hbm, fold_ref), (gain_hbm, gain_ref), (w_in_hbm, w_in_ref),
        (w_out_hbm, w_out_ref), (mix_hbm, mix_ref), (spec_hbm, spec_raw.at[pl.ds(0, spec_hbm.shape[0])]), (table_hbm, table_ref))
    loads = [pltpu.make_async_copy(a, b, local_sem.at[n]) for n, (a, b) in enumerate(whole)]
    groups = channels // step

    def field_load(group):
        some = pl.ds(group * step, step)
        return pltpu.make_async_copy(field_hbm.at[some], field_ref.at[some], local_sem.at[len(whole) + group])

    loads[0].start()
    loads[1].start()
    for group in range(groups):
        field_load(group).start()

    barrier = pltpu.get_barrier_semaphore()
    for k in range(1, lon_n):
        pl.semaphore_signal(barrier, inc=1, device_id={"lon": target(k)})

    @pl.when(lat > 0)
    def _():
        pl.semaphore_signal(barrier, inc=1, device_id={"lat": lat - 1})

    @pl.when(lat < lat_n - 1)
    def _():
        pl.semaphore_signal(barrier, inc=1, device_id={"lat": lat + 1})

    lane = lax.broadcasted_iota(jnp.int32, (rows, LANES), 1)
    half = rows // 2
    loads[1].wait()
    wet = mask_ref[...].astype(F32)

    def mask_group(group):
        for u in range(step):
            c = group * step + u
            if u == 0:
                field_load(group).wait()
            val = field_ref[c].astype(F32) * wet
            at = pl.multiple_of(c * rows, rows)
            parts = [val[:, h * LANES : (h + 1) * LANES] for h in range(tiles)]
            for h in range(tiles):
                flat[h, pl.ds(at, rows), :] = parts[h]
            edge = jnp.where(lane < HALO, parts[0], jnp.where(lane >= LANES - HALO, parts[-1], 0.0))
            edge = edge[:half] + pltpu.roll(edge[half:], LANES - 8 * half, 1)
            for hop in (4, 2, 1):
                edge = edge + pltpu.roll(pltpu.roll(edge, half - hop, 0), LANES - 8 * hop, 1)
            edge32[pl.ds(c, 1), :] = edge[:1]

    first_groups = -(-groups // 2)
    split_at = first_groups * step // 16 * 16
    parts = (slice(0, split_at), slice(split_at, channels))

    def edge_copy(n, way):
        some = pl.ds(parts[n].start, parts[n].stop - parts[n].start)
        put = (edge_right, edge_left)[way]
        return pltpu.make_async_remote_copy(
            edge_mine.at[some], put.at[some], edge_send.at[2 * n + way], edge_recv.at[2 * n + way],
            device_id={"lon": (left, right)[way]})

    def send_edges(n):
        edge_mine[parts[n], :] = edge32[parts[n], :].astype(BF16)
        edge_copy(n, 0).start()
        edge_copy(n, 1).start()

    count = lon_n - 1 + jnp.where(lat > 0, 1, 0) + jnp.where(lat < lat_n - 1, 1, 0)
    pl.loop(0, first_groups)(mask_group)
    pl.semaphore_wait(barrier, count)
    send_edges(0)
    pl.loop(first_groups, groups)(mask_group)
    send_edges(1)
    for load in loads[2:]:
        load.start()

    def own_row(i):
        for h in range(tiles):
            own[i, :, h * LANES : (h + 1) * LANES] = flat[h, pl.ds(i, channels, stride=rows), :].astype(BF16)

    rows_down = pltpu.make_async_remote_copy(
        own.at[pl.ds(0, HALO)], rows_n, rows_send.at[0], rows_recv.at[0], device_id={"lat": lat - 1})
    rows_up = pltpu.make_async_remote_copy(
        own.at[pl.ds(rows - HALO, HALO)], rows_s, rows_send.at[1], rows_recv.at[1], device_id={"lat": lat + 1})
    comb_down = pltpu.make_async_remote_copy(
        comb, comb_n, comb_send.at[0], comb_recv.at[0], device_id={"lat": lat - 1})
    comb_up = pltpu.make_async_remote_copy(
        comb, comb_s, comb_send.at[1], comb_recv.at[1], device_id={"lat": lat + 1})

    def piece(pos):
        return top_all.at[:, :, pl.ds(pl.multiple_of(pos * cols, LANES), cols)]

    def fold_out(j):
        whom = mate_core if j == 0 else lax.rem(chip + j, chips) * 2 + core
        return pltpu.make_async_remote_copy(
            own.at[pl.ds(rows - HALO, HALO)], piece(lon), fold_send.at[j], fold_recv.at[j], device_id={"lon": whom})

    def fold_pass(j):
        pos = lax.rem(chip + chips - j, chips) * 2 + core
        return pltpu.make_async_remote_copy(
            piece(pos), piece(pos), fold_send.at[chips + j - 1], fold_recv.at[chips + j - 1], device_id={"lon": mate_core})

    for i in range(rows - HALO, rows):
        own_row(i)

    @pl.when(lat < lat_n - 1)
    def _():
        rows_up.start()

    @pl.when(lat == lat_n - 1)
    def _():
        for j in range(chips - 1, -1, -1):
            fold_out(j).start()
        top_all[:, :, pl.ds(pl.multiple_of(lon * cols, LANES), cols)] = own[rows - HALO :]

    for i in range(HALO):
        own_row(i)

    @pl.when(lat > 0)
    def _():
        rows_down.start()

    loads[0].wait()
    pattern_t[...] = jnp.zeros(pattern_t.shape, F32)
    for a in range(TAPS):
        for b in range(TAPS):
            pattern_t[b * rows + a : b * rows + a + 1, :channels] = taps_ref[a, b : b + 1, :]
    pattern[...] = pattern_t[...].T[:channels]
    pattern_back[...] = pltpu.roll(pattern[...], LANES - HALO, 1)

    slot = lax.rem(lane, rows)
    index = lax.broadcasted_iota(jnp.int32, (rows, LANES), 0)
    band = jnp.abs(slot - index) <= HALO
    low_slot = slot[:half] < HALO
    high_slot = (slot[:half] >= half + HALO) & (slot[:half] < half + 2 * HALO)

    @pl.loop(0, channels // step)
    def _(group):
        for u in range(step):
            c = group * step + u
            row = jnp.broadcast_to(pattern_back[pl.ds(c, 1), :], (rows, LANES))
            mid = jnp.where(band, pltpu.roll(row, 0, 1, stride=1, stride_axis=0), 0.0)
            row = jnp.broadcast_to(pattern[pl.ds(c, 1), :], (half, LANES))
            far = pltpu.roll(row, 0, 1, stride=1, stride_axis=0)
            far = jnp.concatenate([jnp.where(low_slot, far, 0.0), jnp.where(high_slot, far, 0.0)], axis=0)
            for n, part in enumerate((mid, far)):
                coarse = part.astype(BF16)
                toep[c, 2 * n * rows : (2 * n + 1) * rows, :] = coarse
                toep[c, (2 * n + 1) * rows : (2 * n + 2) * rows, :] = (part - coarse.astype(F32)).astype(BF16)

    halo[...] = jnp.zeros(halo.shape, F32)

    def turned(ref, target_ref):
        n, m = ref.shape
        up = [-(-d // LANES) * LANES for d in (n, m)]
        full = jnp.concatenate([ref[...].astype(F32), jnp.zeros((n, up[1] - m), F32)], axis=1)
        full = jnp.concatenate([full, jnp.zeros((up[0] - n, up[1]), F32)], axis=0)
        target_ref[...] = full.T[: target_ref.shape[0], : target_ref.shape[1]].astype(BF16)

    for n in range(3, 7):
        loads[n].wait()
    turned(w_in_ref, w_in_t)
    w_out_t[...] = jnp.zeros(w_out_t.shape, BF16)
    w_out_t[:, : w_out_ref.shape[1]] = w_out_ref[...]
    turned(mix_ref, mix_t)
    diagonal = lax.broadcasted_iota(jnp.int32, (channels, channels), 0) == lax.broadcasted_iota(
        jnp.int32, (channels, channels), 1)
    gain_col[...] = jnp.broadcast_to(
        jnp.sum(jnp.where(diagonal, gain_ref[...], 0.0), axis=1, keepdims=True), (channels, LANES))

    for i in range(HALO, rows - HALO):
        own_row(i)

    def take_edges(n):
        edge_copy(n, 0).wait()
        edge_copy(n, 1).wait()
        part = parts[n]
        near = lax.rem(lax.broadcasted_iota(jnp.int32, (part.stop - part.start, LANES), 1), 8) < 4
        both = jnp.where(near, edge_right[part, :].astype(F32), edge_left[part, :].astype(F32))
        comb[part, :] = both.astype(BF16)
        comb32[part, :] = both

    def shifted(ring, finish_block):
        high = ring[0].shape[0]
        at = lane[:high]
        blocks = []
        for b in range(TAPS):
            d = b - HALO
            line = []
            for h in range(tiles):
                if d == 0:
                    line.append(ring[h])
                elif d > 0:
                    line.append(pltpu.roll(jnp.where(at < d, ring[h + 1], ring[h]), LANES - d, 1))
                else:
                    line.append(pltpu.roll(jnp.where(at >= LANES + d, ring[h - 1], ring[h]), -d, 1))
            blocks.append(finish_block(jnp.concatenate(line, axis=1)))
        return jnp.concatenate(blocks + [blocks[-1]] * (LANES // rows - TAPS), axis=0)

    blank = jnp.zeros((2 * rows, LANES), BF16)

    def product(c, which, rings, finish_block):
        span = slice(2 * which * rows, 2 * (which + 1) * rows)
        weights = jnp.concatenate(
            [jnp.concatenate([toep[c, span, :], blank], axis=1), jnp.concatenate([blank, toep[c + 1, span, :]], axis=1)],
            axis=0)
        points = jnp.concatenate([shifted(ring, finish_block) for ring in rings], axis=0)
        total = jnp.dot(weights, points, preferred_element_type=F32)
        return total[:rows] + total[rows : 2 * rows], total[2 * rows : 3 * rows] + total[3 * rows :]

    def conv_group(group):
        for u in range(0, step, 2):
            rings = []
            for c in (group * step + u, group * step + u + 1):
                rim = jnp.broadcast_to(comb32[pl.ds(c, 1), :], (rows, LANES))
                rim = pltpu.roll(rim, 0, 1, stride=8, stride_axis=0)
                at = pl.multiple_of(c * rows, rows)
                rings.append([flat[h, pl.ds(at, rows), :].astype(WORK) for h in range(tiles)] + [rim.astype(WORK)])
            totals = product(group * step + u, 0, rings, lambda block: block.astype(BF16))
            for n, total in enumerate(totals):
                at = pl.multiple_of((group * step + u + n) * rows, rows)
                for h in range(tiles):
                    depth[h, pl.ds(at, rows), :] = total[:, h * LANES : (h + 1) * LANES]

    take_edges(0)
    pl.loop(0, split_at // step)(conv_group)
    take_edges(1)

    @pl.when(lat > 0)
    def _():
        comb_down.start()

    @pl.when(lat < lat_n - 1)
    def _():
        comb_up.start()

    pl.loop(split_at // step, groups)(conv_group)

    def edges_of(packed, i):
        return pltpu.roll(packed, 8 * i, 1) if i else packed

    def put_halo(at, value, rim):
        for h in range(tiles):
            halo[h, pl.ds(at, channels, stride=half), :] = value[:, h * LANES : (h + 1) * LANES]
        halo[tiles, pl.ds(at, channels, stride=half), :] = rim

    def await_halo():
        loads[2].wait()

        @pl.when(lat > 0)
        def _():
            rows_down.wait_send()
            comb_down.wait_send()
            rows_up.wait_recv()
            comb_up.wait_recv()
            for r in range(HALO):
                put_halo(r, rows_s[r].astype(F32), edges_of(comb_s[...].astype(F32), rows - HALO + r))

        @pl.when(lat < lat_n - 1)
        def _():
            rows_up.wait_send()
            comb_up.wait_send()
            rows_down.wait_recv()
            comb_down.wait_recv()
            for r in range(HALO):
                put_halo(HALO + r, rows_n[r].astype(F32), edges_of(comb_n[...].astype(F32), r))

        @pl.when(lat == lat_n - 1)
        def _():
            for j in range(1, chips):
                fold_out(j).wait_recv()
                fold_pass(j).start()
            for j in range(chips):
                fold_out(j).wait_send()
            fold_out(0).wait_recv()
            for j in range(1, chips):
                fold_pass(j).wait()
            point = lax.broadcasted_iota(jnp.int32, (lon_points, cols + LANES), 0)
            at = lax.broadcasted_iota(jnp.int32, (1, cols + LANES), 1)
            at = jnp.where(at < cols + HALO, at, at - (cols + LANES)) + lon * cols
            mate = fold_ref[:, :1] - at
            mate = jnp.where(mate < 0, mate + lon_points, mate)
            mate = jnp.where(mate < 0, mate + lon_points, mate)
            mate = jnp.where(mate >= lon_points, mate - lon_points, mate)
            pick = jnp.where(point == mate, 1.0, 0.0).astype(BF16)
            for r in range(HALO):
                row = jnp.dot(top_all[HALO - 1 - r], pick, preferred_element_type=F32)
                put_halo(HALO + r, row[:, :cols], row[:, cols:])

    def halo_conv():
        @pl.loop(0, channels // step)
        def _(group):
            for u in range(0, step, 2):
                rings = []
                for c in (group * step + u, group * step + u + 1):
                    spot = pl.ds(pl.multiple_of(c * half, half), half)
                    rings.append([halo[h, spot, :] for h in range(tiles + 1)])
                totals = product(
                    group * step + u, 1, rings, lambda block: jnp.concatenate([block, block], axis=0).astype(BF16))
                for n, total in enumerate(totals):
                    at = pl.multiple_of((group * step + u + n) * rows, rows)
                    for h in range(tiles):
                        depth[h, pl.ds(at, rows), :] += total[:, h * LANES : (h + 1) * LANES]

    here = pl.ds(pl.multiple_of(lon * cols, LANES), cols)

    def row_at(chunk, q):
        return lax.rem(chunk * lon_n + q + HALO, rows)

    def send_row(chunk, k):
        s = chunk * (lon_n - 1) + lon_n - 1 - k
        return pltpu.make_async_remote_copy(
            res.at[row_at(chunk, target(k))], by_rows.at[chunk, :, here],
            out_send.at[s], out_recv.at[s], device_id={"lon": target(k)})

    def send_back(chunk, k):
        q = target(k)
        s = chunk * (lon_n - 1) + lon_n - 1 - k
        return pltpu.make_async_remote_copy(
            back.at[chunk, :, pl.ds(pl.multiple_of(q * cols, LANES), cols)], spatial.at[chunk * lon_n + lon],
            in_send.at[s], in_recv.at[s], device_id={"lon": q})

    def mix_some(chunk, ks):
        places = [row_at(chunk, target(k)) for k in ks]
        x = jnp.concatenate(
            [depth[h, pl.ds(row, channels, stride=rows), :] for row in places for h in range(tiles)], axis=1)
        mean = jnp.sum(x, axis=0, keepdims=True) * (1.0 / channels)
        centred = x - mean
        var = jnp.sum(centred * centred, axis=0, keepdims=True) * (1.0 / channels)
        gain = jnp.concatenate([gain_col[...]] * (len(ks) * tiles), axis=1)
        normed = (centred * lax.rsqrt(var + 1e-06) * gain).astype(BF16)
        pre = jnp.dot(w_in_t[...], normed, preferred_element_type=F32)
        inner = pre * (GELU_CUBE * (pre * pre) + GELU_LINE)
        hidden = (pre + pre * jnp.tanh(inner)).astype(BF16)
        branch = jnp.dot(w_out_t[...], hidden, preferred_element_type=F32)
        for n, row in enumerate(places):
            wet_row = mask_ref[pl.ds(row, 1), :].astype(F32)
            part = 0.5 * branch[:, n * cols : (n + 1) * cols]
            res[row] = (wet_row * (own[row].astype(F32) + part)).astype(BF16)
        return places

    half_ring = lon_n // 2

    def mix_rows(first, last):
        @pl.loop(first, last)
        def _(at):
            chunk = at // half_ring
            pair = lax.rem(at, half_ring)
            k = lon_n - 1 - 2 * pair
            _, two = mix_some(chunk, (k, k - 1))
            send_row(chunk, k).start()

            @pl.when(pair < half_ring - 1)
            def _():
                send_row(chunk, k - 1).start()

            @pl.when(pair == half_ring - 1)
            def _():
                by_rows[chunk, :, here] = res[two]

    alone = int(half_ring > 1)

    def mix_first(chunk):
        @pl.loop(0, 2 * alone)
        def _(at):
            mix_some(chunk, (lon_n - 1 - at,))
            send_row(chunk, lon_n - 1 - at).start()

    def spectral(chunk):
        for k in range(lon_n - 1, 0, -1):
            send_row(chunk, k).wait_recv()
        spectrum = jnp.dot(by_rows[chunk], table_ref[...], preferred_element_type=F32)
        s_re = spectrum[:, :modes]
        s_im = spectrum[:, modes:]
        g_re = spec_ref[0]
        g_im = spec_ref[1]
        scaled = jnp.concatenate(
            [(g_re * s_re - g_im * s_im).astype(BF16), (g_re * s_im + g_im * s_re).astype(BF16)], axis=1)
        back[chunk] = lax.dot_general(
            scaled, table_ref[...], (((1,), (1,)), ((), ())), preferred_element_type=F32).astype(BF16)
        for k in range(lon_n - 1, 0, -1):
            send_back(chunk, k).start()
        spatial[chunk * lon_n + lon] = back[chunk, :, here]

    def finish(chunk):
        @pl.loop(0, lon_n // 2)
        def _(pair):
            k = 2 * pair

            @pl.when(pair > 0)
            def _():
                send_back(chunk, k).wait_recv()

            send_back(chunk, k + 1).wait_recv()
            spots = [source(k), source(k + 1)]
            points = jnp.concatenate([spatial[chunk * lon_n + pos] for pos in spots], axis=1)
            mixed = jnp.dot(mix_t[...], points, preferred_element_type=F32)
            for n, pos in enumerate(spots):
                row = row_at(chunk, pos)
                wet_row = mask_ref[pl.ds(row, 1), :].astype(F32)
                val = wet_row * (res[row].astype(F32) + mixed[:, n * cols : (n + 1) * cols])
                for h in range(tiles):
                    flat_out[h, pl.ds(row, channels, stride=rows), :] = val[:, h * LANES : (h + 1) * LANES]

    needs = [
        any((chunk * lon_n + q + HALO) % rows < HALO or (chunk * lon_n + q + HALO) % rows >= rows - HALO for q in range(lon_n))
        for chunk in range(per)]
    early = needs.index(True)
    if early:
        mix_first(0)
        mix_rows(alone, early * half_ring)
    loads[7].wait()
    wide = modes // LANES
    for p in range(2):
        for t in range(wide):
            spec_ref[p, :, t * LANES : (t + 1) * LANES] = spec_raw[pl.ds(2 * t + p, channels, stride=2 * wide), :]
    loads[8].wait()
    if early > 1:
        pl.loop(0, early - 1)(spectral)
    await_halo()
    if early:
        spectral(early - 1)
    halo_conv()
    mix_first(early)
    mix_rows(early * half_ring + alone, per * half_ring)
    pl.loop(early, per)(spectral)
    if per > 1:
        pl.loop(0, per - 1)(finish)

    @pl.loop(0, per * (lon_n - 1))
    def _(at):
        chunk = at // (lon_n - 1)
        k = lon_n - 1 - lax.rem(at, lon_n - 1)
        send_row(chunk, k).wait_send()
        send_back(chunk, k).wait_send()

    finish(per - 1)

    @pl.loop(0, channels // step)
    def _(group):
        for u in range(step):
            c = group * step + u
            at = pl.multiple_of(c * rows, rows)
            for h in range(tiles):
                out_ref[c, :, h * LANES : (h + 1) * LANES] = flat_out[h, pl.ds(at, rows), :].astype(BF16)


def local(lat_n, lon_n, field, land_mask, fold_partner, dw_kernel, norm_gain, w_in, w_out, spec_gain, mix_weight):
    channels, rows, cols = field.shape
    modes = spec_gain.shape[2]
    hid = w_in.shape[1]
    lon_points = cols * lon_n
    hid_up = -(-hid // 16) * 16
    chan_up = -(-channels // LANES) * LANES
    tiles = cols // LANES
    table = jnp.asarray(dft_table(lon_points, modes))
    taps = dw_kernel.transpose(1, 2, 0)
    wide = modes // LANES
    spec = spec_gain.transpose(1, 0, 2).reshape(channels, 2, wide, LANES).transpose(0, 2, 1, 3).reshape(-1, LANES)
    room = -(-channels // 16) * 16
    per = rows // lon_n
    groups = channels // loop_step(channels)
    sizes = (channels, rows, cols, lat_n, lon_n, modes)
    operands = (field, land_mask, fold_partner[None, :], taps, norm_gain[None, :], w_in, w_out.T, mix_weight, spec, table)
    dma = pltpu.SemaphoreType.DMA
    peers = lon_n - 1
    return pl.pallas_call(
        functools.partial(kernel, sizes),
        out_shape=pltpu.VMEM(field.shape, BF16),
        in_specs=[pl.BlockSpec(memory_space=pltpu.HBM)] * len(operands),
        out_specs=pl.BlockSpec(memory_space=pltpu.VMEM),
        scratch_shapes=[
            *[pltpu.VMEM(x.shape, x.dtype) for x in operands[:-2]],
            pltpu.VMEM((room * 2 * wide, LANES), F32),
            pltpu.VMEM(table.shape, BF16),
            pltpu.VMEM((tiles, room * rows, LANES), F32),
            pltpu.VMEM((rows, channels, cols), BF16),
            pltpu.VMEM((tiles, room * rows, LANES), F32),
            pltpu.VMEM((tiles, room * rows, LANES), F32),
            pltpu.VMEM((tiles + 1, room * rows // 2, LANES), F32),
            pltpu.VMEM((channels, 4 * rows, LANES), BF16),
            pltpu.VMEM((LANES, chan_up), F32),
            *[pltpu.VMEM((channels, LANES), F32)] * 4,
            pltpu.VMEM((rows, channels, cols), BF16),
            pltpu.VMEM((per, channels, lon_points), BF16),
            pltpu.VMEM((per, channels, lon_points), BF16),
            pltpu.VMEM((rows, channels, cols), BF16),
            *[pltpu.VMEM((channels, LANES), BF16)] * 6,
            *[pltpu.VMEM((HALO, channels, cols), BF16)] * 2,
            pltpu.VMEM((HALO, channels, lon_points), BF16),
            pltpu.VMEM(spec_gain.shape, F32),
            pltpu.VMEM((hid_up, channels), BF16),
            pltpu.VMEM((channels, hid_up), BF16),
            pltpu.VMEM((channels, channels), BF16),
            pltpu.VMEM((channels, LANES), F32),
            dma((len(operands) + groups,)),
            *[dma((4,))] * 2,
            *[dma((2,))] * 4,
            *[dma((peers,))] * 2,
            *[dma((peers * per,))] * 4,
        ],
        compiler_params=pltpu.CompilerParams(
            collective_id=0, has_side_effects=True, vmem_limit_bytes=VMEM_LIMIT),
        name="block",
    )(*operands)


def solution(mesh):
    placed = (P(None, "lat", "lon"), P("lat", "lon"), P(), P(), P(), P(), P(), P(), P())
    return jax.shard_map(
        functools.partial(local, mesh.shape["lat"], mesh.shape["lon"]),
        mesh=mesh, in_specs=placed, out_specs=P(None, "lat", "lon"), check_vma=False,
    )
```
